32 devices in a mesh: gx: 32 (over z, y, x, core).
Axes of the slice: x: 2, y: 2, z: 4, core: 2. Of those that a mesh axis runs over, the one named last changes fastest.
Arguments:
- fine: bfloat16 [64, 8192, 128], P(None, 'gx'), may hold values from -6 to 6
- pattern: int32 [8, 8192], P(None, 'gx'), may hold values from 0 to 3
- stencil: bfloat16 [3, 128, 128], replicated, may hold values from -0.3125 to 0.3125
- restrict: bfloat16 [8, 4, 128, 128], replicated, may hold values from -0.5 to 0.5
- coarse_inv: bfloat16 [8, 128, 128], replicated, may hold values from -0.5 to 0.5
Outputs:
- smoothed: float32 [64, 8192, 128], P(None, 'gx')
The draws below stay inside these ranges and needn't reach their ends.
All inputs are finite; a program needn't handle non-finite values.
Results may differ from the reference program's by a relative error of at most 0.0046.
Values may be sent and summed in bfloat16 or wider, within the bound.
A program may use at most 128 MiB of HBM per device.

```python
import jax
import jax.numpy as jnp
from jax import lax

WIDTH = 128
KINDS = 4
LEVELS = 8
BLK_DEV = 256
NVEC = 64
NB = 8192


def touch_ends(values, rng, least, high):
    place = [jax.random.randint(jax.random.fold_in(rng, axis), (), 0, length) for axis, length in enumerate(values.shape)]
    widest = values.shape.index(max(values.shape))
    next_to = place[:widest] + [(place[widest] + 1) % values.shape[widest]] + place[widest + 1:]
    return values.at[tuple(place)].set(least).at[tuple(next_to)].set(high)


def block_levels(key, shape, pieces, low, top_value):
    def one(axis_at, parts):
        steps = jax.random.uniform(jax.random.fold_in(jax.random.fold_in(key, 6), axis_at), (parts,), jnp.float32, low / len(pieces), top_value / len(pieces))
        return jnp.repeat(jnp.exp(steps), shape[axis_at] // parts).reshape((-1,) + (1,) * (len(shape) - axis_at - 1))

    factor_of = one(*pieces[0])
    for cut in pieces[1:]:
        factor_of = factor_of * one(*cut)
    return factor_of


def gaussian(rng, dims, scale, reach, cuts=(), held_as=jnp.bfloat16):
    values = jax.random.normal(rng, dims, jnp.float32) * scale
    if len(cuts) > 0:
        values = block_levels(rng, dims, cuts, -0.22, 0.18) * values
    return jnp.clip(values, min=-reach, max=reach).astype(held_as)


def setup_inputs(seed: int = 0) -> dict:
    key_list = jax.random.split(jax.random.key(seed), 6)
    fine = gaussian(key_list[0], (NVEC, NB, WIDTH), 1.0, 6.0, ((1, 32),))
    pattern = touch_ends(jax.random.randint(key_list[1], (LEVELS, NB), 0, KINDS), jax.random.fold_in(key_list[1], 1), 0, KINDS - 1).astype(jnp.int32)
    stencil = gaussian(key_list[2], (3, WIDTH, WIDTH), (3 * WIDTH) ** -0.5, 0.3125)
    restrict = gaussian(key_list[3], (LEVELS, KINDS, WIDTH, WIDTH), WIDTH ** -0.5, 0.5)
    coarse_inv = gaussian(key_list[4], (LEVELS, WIDTH, WIDTH), WIDTH ** -0.5, 0.5)
    return {"fine": fine, "pattern": pattern, "stencil": stencil, "restrict": restrict, "coarse_inv": coarse_inv}


EXACT = lax.Precision.HIGHEST


def one_vector(fine_vec, pattern, stencil, restrict, coarse_inv):
    all_blocks = fine_vec.shape[0]
    width = fine_vec.shape[1]
    earlier = jnp.roll(fine_vec, 1, axis=0)
    later = jnp.roll(fine_vec, -1, axis=0)
    result = jnp.dot(earlier, stencil[0], preferred_element_type=jnp.float32)
    result = result + jnp.dot(fine_vec, stencil[1], preferred_element_type=jnp.float32)
    result = result + jnp.dot(later, stencil[2], preferred_element_type=jnp.float32)
    widened = fine_vec.astype(jnp.float32)
    kinds_row = jnp.arange(KINDS, dtype=jnp.int32)
    for level_num in range(LEVELS):
        coarse_num = max(all_blocks // 4 ** (level_num + 1), 1)
        span_blocks = all_blocks // coarse_num
        run_len = min(span_blocks, BLK_DEV)
        run_num = all_blocks // run_len
        selector = pattern[level_num][:, None] == kinds_row[None, :]
        onehot = selector.astype(jnp.float32).reshape(run_num, run_len, KINDS)
        tiles = restrict[level_num].astype(jnp.float32)
        grouped = jnp.einsum("nsc,nsk->nkc", widened.reshape(run_num, run_len, width), onehot, precision=EXACT)
        grouped = grouped.astype(jnp.bfloat16).astype(jnp.float32)
        per_run = jnp.einsum("nkc,kcd->nd", grouped, tiles, precision=EXACT)
        coarse = jnp.sum(per_run.reshape(coarse_num, span_blocks // run_len, width), axis=1) * (span_blocks ** -0.5)
        rounded = coarse.astype(jnp.bfloat16)
        solved = jnp.dot(rounded, coarse_inv[level_num], preferred_element_type=jnp.float32).astype(jnp.bfloat16)
        lifted = jnp.einsum("jd,kcd->jkc", solved.astype(jnp.float32), tiles, precision=EXACT)
        kind_map = pattern[level_num].reshape(coarse_num, span_blocks)
        for kind_num in range(KINDS):
            chosen = (kind_map == kind_num)[:, :, None]
            part_add = jnp.where(chosen, lifted[:, kind_num][:, None, :], jnp.float32(0.0))
            result = result + part_add.reshape(all_blocks, width)
    return result


def reference(fine, pattern, stencil, restrict, coarse_inv):
    return lax.map(lambda fine_vec: one_vector(fine_vec, pattern, stencil, restrict, coarse_inv), fine)
```

```python
import functools

import jax
import jax.numpy as jnp
from jax import lax
from jax.experimental import pallas as pl
from jax.experimental.pallas import tpu as pltpu
from jax.sharding import PartitionSpec as P

MESH = pl.DeviceIdType.MESH
F32 = jnp.float32
BF16 = jnp.bfloat16
TILE = 16
VMEM_LIMIT = 30 * 2**20


def round_up(value, unit):
    return -(-value // unit) * unit


class Plan:
    def __init__(self, devices, vectors, blocks, width, levels, kinds):
        self.devices, self.vectors, self.blocks = devices, vectors, blocks
        self.width, self.levels, self.kinds = width, levels, kinds
        all_blocks = devices * blocks
        self.spans, self.local_spans, self.counts, self.groups = [], [], [], []
        for level in range(levels):
            span = all_blocks // max(all_blocks // 4 ** (level + 1), 1)
            local = min(span, blocks)
            self.spans.append(span)
            self.local_spans.append(local)
            self.counts.append(blocks // local)
            self.groups.append(span // local)
        self.narrow = [l for l in range(levels) if self.counts[l] > 1]
        self.wide = [l for l in range(levels) if self.counts[l] == 1]
        self.crossing = [l for l in range(levels) if self.groups[l] > 1]
        self.padded = {l: round_up(self.counts[l], TILE) for l in self.narrow}
        self.offsets, at = {}, 0
        for l in self.narrow:
            self.offsets[l] = at
            at += kinds * self.padded[l]
        self.narrow_rows = at
        self.wide_used = len(self.wide) * kinds + 2
        self.wide_rows = round_up(self.wide_used, TILE)


def wide_rows_onehot(plan, pattern, rows_axis):
    shape = (plan.wide_rows, plan.blocks) if rows_axis == 0 else (plan.blocks, plan.wide_rows)
    row = lax.broadcasted_iota(jnp.int32, shape, rows_axis)
    block = lax.broadcasted_iota(jnp.int32, shape, 1 - rows_axis)
    base = len(plan.wide) * plan.kinds
    hit = ((row == base) & (block == 0)) | ((row == base + 1) & (block == plan.blocks - 1))
    for position, level in enumerate(plan.wide):
        kinds = pattern[level : level + 1, :] if rows_axis == 0 else pattern[:, level : level + 1]
        first = position * plan.kinds
        inside = (row >= first) & (row < first + plan.kinds)
        hit = hit | (inside & (row - first == kinds))
    return hit.astype(F32).astype(BF16)


def narrow_onehot(plan, pattern, level, rows_axis):
    padded = plan.padded[level]
    rows = plan.kinds * padded
    shape = (rows, plan.blocks) if rows_axis == 0 else (plan.blocks, rows)
    row = lax.broadcasted_iota(jnp.int32, shape, rows_axis)
    block = lax.broadcasted_iota(jnp.int32, shape, 1 - rows_axis)
    kinds = pattern[level : level + 1, :] if rows_axis == 0 else pattern[:, level : level + 1]
    target = kinds * padded + block // plan.local_spans[level]
    return (row == target).astype(F32).astype(BF16)

PITCH = 40


def exchange_kernel(plan, chunk, pattern_hbm, fine_hbm, restrict_hbm, inverse_hbm, stencil_hbm,
                    table_ref, level0_ref, spread_ref,
                    pattern_ref, fine_ref, restrict_ref, inverse_ref, stencil_ref, wide_f32, wide_onehot, onehot, few,
                    grouped, rows, coarse_ref, halo_ref, beside_ref, before, after,
                    from_group, to_column, from_column, to_group, back,
                    fine_sem, weight_sem, group_send, group_recv,
                    column_send, column_recv, back_send, back_recv, halo_send, halo_recv):
    width, kinds, blocks = plan.width, plan.kinds, plan.blocks
    load = 16
    loads = plan.vectors // load
    steps = plan.vectors // chunk
    devices = plan.devices
    near = plan.groups[plan.crossing[0]]
    far = devices // near
    local = len(plan.wide) - len(plan.crossing)
    crossing = len(plan.crossing)
    part = plan.vectors // near
    me = lax.axis_index("gx")
    mine = lax.rem(me, near)
    place = me // near

    def chunk_of(step):
        return pl.ds(pl.multiple_of(step * chunk, chunk), chunk)

    def fine_copy(step):
        here = pl.ds(step * load, load)
        return pltpu.make_async_copy(fine_hbm.at[here], fine_ref.at[here], fine_sem.at[step])

    wide_first = plan.wide[0]
    wide_weights = pl.ds(wide_first, len(plan.wide))
    weight_copies = [
        pltpu.make_async_copy(restrict_hbm.at[wide_weights], restrict_ref.at[wide_weights], weight_sem.at[0]),
        pltpu.make_async_copy(restrict_hbm.at[pl.ds(0, wide_first)], restrict_ref.at[pl.ds(0, wide_first)], weight_sem.at[1]),
        pltpu.make_async_copy(inverse_hbm, inverse_ref, weight_sem.at[2]),
        pltpu.make_async_copy(stencil_hbm, stencil_ref, weight_sem.at[3]),
    ]
    pattern_copy = pltpu.make_async_copy(pattern_hbm, pattern_ref, weight_sem.at[4])
    pattern_copy.start()
    for step in range(loads - 1):
        fine_copy(step).start()
    weight_copies[0].start()
    fine_copy(loads - 1).start()
    for copy in weight_copies[1:]:
        copy.start()

    def group_peer(apart):
        return place * near + lax.rem(mine + apart, near)

    def column_peer(apart):
        return lax.rem(place + apart, far) * near + mine

    nexts = lax.rem(me + 1, devices)
    previous = lax.rem(me + devices - 1, devices)
    barrier = pltpu.get_barrier_semaphore()
    peers = [group_peer(a) for a in range(1, near)] + [column_peer(a) for a in range(1, far)] + [nexts, previous]
    for peer in peers:
        pl.semaphore_signal(barrier, inc=1, device_id=(peer,), device_id_type=MESH)

    pattern_copy.wait()
    wide_onehot[...] = wide_rows_onehot(plan, pattern_ref[...], 0)

    for step in range(loads):
        fine_copy(step).wait()
        here = pl.ds(step * load, load)
        for first in range(0, load, 2):
            at = step * load + first
            both = jnp.concatenate([fine_ref[at], fine_ref[at + 1]], axis=1)
            both = jnp.dot(wide_onehot[...], both, preferred_element_type=F32)
            few[first, pl.ds(0, plan.wide_rows), :] = both[:, :width]
            few[first + 1, pl.ds(0, plan.wide_rows), :] = both[:, width:]
        for row in range(plan.wide_used):
            rows[row, here, :] = few[:, row, :].astype(BF16)
    weight_copies[0].wait()
    for position, level in enumerate(plan.wide):
        first = position * kinds
        joined = jnp.concatenate([rows[first + kind] for kind in range(kinds)], axis=1)
        coarse = jnp.dot(joined, restrict_ref[level], preferred_element_type=F32)
        coarse_ref[position] = (coarse * plan.spans[level] ** (-0.5)).astype(BF16)
    base = len(plan.wide) * kinds
    halo_ref[0] = rows[base]
    halo_ref[1] = rows[base + 1]

    pl.semaphore_wait(barrier, len(peers))

    def part_of(index):
        return pl.ds(pl.multiple_of(index * part, part), part)

    copies = []
    for apart in range(1, near):
        theirs = lax.rem(mine + apart, near)
        copies.append(pltpu.make_async_remote_copy(
            src_ref=coarse_ref.at[pl.ds(local, crossing), part_of(theirs), :],
            dst_ref=from_group.at[apart],
            send_sem=group_send.at[apart], recv_sem=group_recv.at[apart],
            device_id=(group_peer(apart),), device_id_type=MESH))
    halo_copies = []
    for side, peer in ((0, previous), (1, nexts)):
        halo_copies.append(pltpu.make_async_remote_copy(
            src_ref=halo_ref.at[side], dst_ref=beside_ref.at[1 - side],
            send_sem=halo_send.at[side], recv_sem=halo_recv.at[1 - side],
            device_id=(peer,), device_id_type=MESH))
    for copy in copies + halo_copies:
        copy.start()

    for level in plan.narrow:
        onehot[pl.ds(plan.offsets[level], kinds * plan.padded[level]), :] = narrow_onehot(
            plan, pattern_ref[...], level, 0)
    turned = pattern_ref[...].T
    for level in plan.narrow:
        columns = pl.ds(plan.offsets[level], kinds * plan.padded[level])
        spread_ref[:, columns] = narrow_onehot(plan, turned, level, 1)
    spread_ref[:, pl.ds(plan.narrow_rows, plan.wide_rows)] = wide_rows_onehot(plan, turned, 1)
    before[:, pl.ds(0, 8), :] = jnp.zeros((2, 8, width), F32)
    after[:, pl.ds(blocks, 8), :] = jnp.zeros((2, 8, width), F32)
    for copy in weight_copies[1:]:
        copy.wait()

    def narrow(step, _):
        here = chunk_of(step)
        stencils = jnp.concatenate([stencil_ref[0], stencil_ref[1], stencil_ref[2]], axis=1)
        for first in range(0, chunk, 2):
            at = step * chunk + first
            both = jnp.concatenate([fine_ref[at], fine_ref[at + 1]], axis=1)
            both = jnp.dot(onehot[...], both, preferred_element_type=F32).astype(BF16)
            grouped[first] = both[:, :width]
            grouped[first + 1] = both[:, width:]
        for slot in range(chunk):
            at = step * chunk + slot
            three = jnp.dot(fine_ref[at], stencils, preferred_element_type=F32)
            turn = slot % 2
            before[turn, pl.ds(8, blocks), :] = three[:, :width]
            after[turn, pl.ds(0, blocks), :] = three[:, 2 * width :]
            level0_ref[at] = (three[:, width : 2 * width] + before[turn, pl.ds(7, blocks), :]
                              + after[turn, pl.ds(1, blocks), :])
        for level in plan.narrow:
            padded = plan.padded[level]
            slices = [pl.ds(plan.offsets[level] + kind * padded, padded) for kind in range(kinds)]
            joined = jnp.concatenate(
                [grouped[:, tile, :].reshape(chunk * padded, width) for tile in slices], axis=1)
            coarse = jnp.dot(joined, restrict_ref[level], preferred_element_type=F32)
            rounded = (coarse * plan.spans[level] ** (-0.5)).astype(BF16)
            solved = jnp.dot(rounded, inverse_ref[level], preferred_element_type=F32).astype(BF16)
            lifted = lax.dot_general(
                solved, restrict_ref[level], (((1,), (1,)), ((), ())), preferred_element_type=F32).astype(BF16)
            for kind, tile in enumerate(slices):
                table_ref[here, tile, :] = lifted[:, kind * width : (kind + 1) * width].reshape(chunk, padded, width)
        return 0

    def lift_wide(position, rounded):
        level = plan.wide[position]
        solved = jnp.dot(rounded, inverse_ref[level], preferred_element_type=F32).astype(BF16)
        lifted = lax.dot_general(
            solved, restrict_ref[level], (((1,), (1,)), ((), ())), preferred_element_type=F32)
        for kind in range(kinds):
            wide_f32[:, position * kinds + kind, :] = lifted[:, kind * width : (kind + 1) * width]

    first_stop = steps // 4
    second_stop = steps // 2
    lax.fori_loop(0, first_stop, narrow, 0)

    total = coarse_ref[pl.ds(local, crossing), part_of(mine), :].astype(F32)
    for apart, copy in enumerate(copies, 1):
        copy.wait_recv()
        total = total + from_group[apart].astype(F32)
    to_column[...] = total.astype(BF16)

    column_copies = []
    for apart in range(1, far):
        column_copies.append(pltpu.make_async_remote_copy(
            src_ref=to_column.at[pl.ds(1, crossing - 1)], dst_ref=from_column.at[apart],
            send_sem=column_send.at[apart], recv_sem=column_recv.at[apart],
            device_id=(column_peer(apart),), device_id_type=MESH))
    for copy in column_copies:
        copy.start()

    for copy in halo_copies:
        copy.wait_recv()
    for row in range(plan.wide_used, plan.wide_rows):
        wide_f32[:, row, :] = jnp.zeros((plan.vectors, width), F32)
    wide_f32[:, base, :] = jnp.dot(beside_ref[0], stencil_ref[0], preferred_element_type=F32)
    wide_f32[:, base + 1, :] = jnp.dot(beside_ref[1], stencil_ref[2], preferred_element_type=F32)
    for position in range(local):
        lift_wide(position, coarse_ref[position])
    lax.fori_loop(first_stop, second_stop, narrow, 0)

    to_group[0] = to_column[0]
    sums = [to_column[index].astype(F32) for index in range(crossing)]
    for apart, copy in enumerate(column_copies, 1):
        copy.wait_recv()
        source = lax.rem(place + far - apart, far)
        for index in range(1, crossing):
            reach = plan.groups[plan.crossing[index]] // near
            keep = (source // reach == place // reach).astype(F32)
            sums[index] = sums[index] + keep * from_column[apart, index - 1].astype(F32)
    for index in range(1, crossing):
        to_group[index] = sums[index].astype(BF16)

    back_copies = []
    for apart in range(1, near):
        back_copies.append(pltpu.make_async_remote_copy(
            src_ref=to_group, dst_ref=back.at[apart],
            send_sem=back_send.at[apart], recv_sem=back_recv.at[apart],
            device_id=(group_peer(apart),), device_id_type=MESH))
    for copy in back_copies:
        copy.start()

    lax.fori_loop(second_stop, steps, narrow, 0)
    for copy in copies:
        copy.wait_send()
    coarse_ref[pl.ds(local, crossing), part_of(mine), :] = to_group[...]
    for apart, copy in enumerate(back_copies, 1):
        copy.wait_recv()
        source = lax.rem(mine + near - apart, near)
        coarse_ref[pl.ds(local, crossing), part_of(source), :] = back[apart]
    for position in range(local, len(plan.wide)):
        lift_wide(position, coarse_ref[position])
    table_ref[:, pl.ds(plan.narrow_rows, plan.wide_rows), :] = wide_f32[:, pl.ds(0, plan.wide_rows), :].astype(BF16)
    for copy in halo_copies + column_copies + back_copies:
        copy.wait_send()


def final_kernel(plan, pieces, spread_ref, table_ref, level0_ref, out_hbm, staged, out_sem):
    width = plan.width
    copies, at = [], 0
    for index, piece in enumerate(pieces):
        for first in range(at, at + piece, 2):
            tables = jnp.concatenate([table_ref[first], table_ref[first + 1]], axis=1)
            both = jnp.dot(spread_ref[...], tables, preferred_element_type=F32)
            staged[first] = both[:, :width] + level0_ref[first]
            staged[first + 1] = both[:, width:] + level0_ref[first + 1]
        here = pl.ds(at, piece)
        copy = pltpu.make_async_copy(staged.at[here], out_hbm.at[here], out_sem.at[index])
        copy.start()
        copies.append(copy)
        at += piece
    for copy in copies:
        copy.wait()


def shards(fine, pattern, stencil, restrict, coarse_inv):
    devices = lax.axis_size("gx")
    vectors, blocks, width = fine.shape
    levels, kinds = restrict.shape[:2]
    plan = Plan(devices, vectors, blocks, width, levels, kinds)
    stacked = restrict.reshape(levels, kinds * width, width)
    wide_count = len(plan.wide)
    chunk = 8
    near = plan.groups[plan.crossing[0]]
    far = devices // near
    crossing = len(plan.crossing)
    part = vectors // near
    table_rows = plan.narrow_rows + plan.wide_rows
    vmem = pl.BlockSpec(memory_space=pltpu.VMEM)
    hbm = pl.BlockSpec(memory_space=pltpu.HBM)
    dma = pltpu.SemaphoreType.DMA
    pinned = [pltpu.with_memory_space_constraint(x, pltpu.HBM) for x in (pattern, fine, stacked, coarse_inv, stencil)]
    table, level0, spread = pl.pallas_call(
        functools.partial(exchange_kernel, plan, chunk),
        out_shape=(
            pltpu.VMEM((vectors, table_rows, width), BF16),
            pltpu.VMEM((vectors, blocks, width), F32),
            pltpu.VMEM((blocks, table_rows), BF16),
        ),
        in_specs=[hbm] * 5,
        out_specs=(vmem, vmem, vmem),
        scratch_shapes=[
            pltpu.VMEM(pattern.shape, jnp.int32),
            pltpu.VMEM(fine.shape, BF16),
            pltpu.VMEM(stacked.shape, BF16),
            pltpu.VMEM(coarse_inv.shape, BF16),
            pltpu.VMEM(stencil.shape, BF16),
            pltpu.VMEM((vectors, PITCH, width), F32),
            pltpu.VMEM((plan.wide_rows, blocks), BF16),
            pltpu.VMEM((plan.narrow_rows, blocks), BF16),
            pltpu.VMEM((16, PITCH, width), F32),
            pltpu.VMEM((chunk, plan.narrow_rows, width), BF16),
            pltpu.VMEM((plan.wide_used, vectors, width), BF16),
            pltpu.VMEM((wide_count, vectors, width), BF16),
            pltpu.VMEM((2, vectors, width), BF16),
            pltpu.VMEM((2, vectors, width), BF16),
            pltpu.VMEM((2, blocks + 8, width), F32),
            pltpu.VMEM((2, blocks + 8, width), F32),
            pltpu.VMEM((near, crossing, part, width), BF16),
            pltpu.VMEM((crossing, part, width), BF16),
            pltpu.VMEM((far, crossing - 1, part, width), BF16),
            pltpu.VMEM((crossing, part, width), BF16),
            pltpu.VMEM((near, crossing, part, width), BF16),
            dma((vectors // 16,)), dma((5,)),
            dma((near,)), dma((near,)), dma((far,)), dma((far,)), dma((near,)), dma((near,)), dma((2,)), dma((2,)),
        ],
        compiler_params=pltpu.CompilerParams(
            collective_id=0, has_side_effects=True, vmem_limit_bytes=VMEM_LIMIT),
        name="exchange",
    )(*pinned)

    pieces = [8] * (vectors // 8 - 1) + [4, 2, 2]
    return pl.pallas_call(
        functools.partial(final_kernel, plan, pieces),
        out_shape=jax.ShapeDtypeStruct(fine.shape, F32),
        in_specs=[vmem, vmem, vmem],
        out_specs=pl.BlockSpec(memory_space=pl.ANY),
        scratch_shapes=[pltpu.VMEM(fine.shape, F32), dma((len(pieces),))],
        compiler_params=pltpu.CompilerParams(vmem_limit_bytes=VMEM_LIMIT),
        name="final",
    )(spread, table, level0)


def solution(mesh):
    in_specs = (P(None, "gx", None), P(None, "gx"), P(), P(), P())
    out_specs = P(None, "gx", None)
    return jax.shard_map(shards, mesh=mesh, in_specs=in_specs, out_specs=out_specs, check_vma=False)
```

```python
import functools

import jax
import jax.numpy as jnp
from jax import lax
from jax.experimental import pallas as pl
from jax.experimental.pallas import tpu as pltpu
from jax.sharding import PartitionSpec as P

MESH = pl.DeviceIdType.MESH
F32 = jnp.float32
BF16 = jnp.bfloat16
TILE = 16
VMEM_LIMIT = 30 * 2**20


def round_up(value, unit):
    return -(-value // unit) * unit


class Plan:
    def __init__(self, devices, vectors, blocks, width, levels, kinds):
        self.devices, self.vectors, self.blocks = devices, vectors, blocks
        self.width, self.levels, self.kinds = width, levels, kinds
        all_blocks = devices * blocks
        self.spans, self.local_spans, self.counts, self.groups = [], [], [], []
        for level in range(levels):
            span = all_blocks // max(all_blocks // 4 ** (level + 1), 1)
            local = min(span, blocks)
            self.spans.append(span)
            self.local_spans.append(local)
            self.counts.append(blocks // local)
            self.groups.append(span // local)
        self.narrow = [l for l in range(levels) if self.counts[l] > 1]
        self.wide = [l for l in range(levels) if self.counts[l] == 1]
        self.crossing = [l for l in range(levels) if self.groups[l] > 1]
        self.padded = {l: round_up(self.counts[l], TILE) for l in self.narrow}
        self.offsets, at = {}, 0
        for l in self.narrow:
            self.offsets[l] = at
            at += kinds * self.padded[l]
        self.narrow_rows = at
        self.wide_used = len(self.wide) * kinds + 2
        self.wide_rows = round_up(self.wide_used, TILE)


def wide_rows_onehot(plan, pattern, rows_axis):
    shape = (plan.wide_rows, plan.blocks) if rows_axis == 0 else (plan.blocks, plan.wide_rows)
    row = lax.broadcasted_iota(jnp.int32, shape, rows_axis)
    block = lax.broadcasted_iota(jnp.int32, shape, 1 - rows_axis)
    base = len(plan.wide) * plan.kinds
    hit = ((row == base) & (block == 0)) | ((row == base + 1) & (block == plan.blocks - 1))
    for position, level in enumerate(plan.wide):
        kinds = pattern[level : level + 1, :] if rows_axis == 0 else pattern[:, level : level + 1]
        first = position * plan.kinds
        inside = (row >= first) & (row < first + plan.kinds)
        hit = hit | (inside & (row - first == kinds))
    return hit.astype(F32).astype(BF16)


def narrow_onehot(plan, pattern, level, rows_axis):
    padded = plan.padded[level]
    rows = plan.kinds * padded
    shape = (rows, plan.blocks) if rows_axis == 0 else (plan.blocks, rows)
    row = lax.broadcasted_iota(jnp.int32, shape, rows_axis)
    block = lax.broadcasted_iota(jnp.int32, shape, 1 - rows_axis)
    kinds = pattern[level : level + 1, :] if rows_axis == 0 else pattern[:, level : level + 1]
    target = kinds * padded + block // plan.local_spans[level]
    return (row == target).astype(F32).astype(BF16)

PITCH = 40


def exchange_kernel(plan, chunk, pattern_hbm, fine_hbm, restrict_hbm, inverse_hbm, stencil_hbm,
                    table_ref, level0_ref, spread_ref,
                    pattern_ref, fine_ref, restrict_ref, inverse_ref, stencil_ref, wide_f32, wide_onehot, onehot, few,
                    grouped, joint, rows, coarse_ref, halo_ref, beside_ref,
                    from_group, to_column, from_column, to_group, back,
                    fine_sem, weight_sem, group_send, group_recv,
                    column_send, column_recv, back_send, back_recv, halo_send, halo_recv):
    width, kinds, blocks = plan.width, plan.kinds, plan.blocks
    load = 16
    loads = plan.vectors // load
    steps = plan.vectors // chunk
    devices = plan.devices
    near = plan.groups[plan.crossing[0]]
    far = devices // near
    local = len(plan.wide) - len(plan.crossing)
    crossing = len(plan.crossing)
    part = plan.vectors // near
    me = lax.axis_index("gx")
    mine = lax.rem(me, near)
    place = me // near

    def chunk_of(step):
        return pl.ds(pl.multiple_of(step * chunk, chunk), chunk)

    def fine_copy(step):
        here = pl.ds(step * load, load)
        return pltpu.make_async_copy(fine_hbm.at[here], fine_ref.at[here], fine_sem.at[step])

    wide_first = plan.wide[0]
    wide_weights = pl.ds(wide_first, len(plan.wide))
    weight_copies = [
        pltpu.make_async_copy(restrict_hbm.at[wide_weights], restrict_ref.at[wide_weights], weight_sem.at[0]),
        pltpu.make_async_copy(restrict_hbm.at[pl.ds(0, wide_first)], restrict_ref.at[pl.ds(0, wide_first)], weight_sem.at[1]),
        pltpu.make_async_copy(inverse_hbm, inverse_ref, weight_sem.at[2]),
        pltpu.make_async_copy(stencil_hbm, stencil_ref, weight_sem.at[3]),
    ]
    pattern_copy = pltpu.make_async_copy(pattern_hbm, pattern_ref, weight_sem.at[4])
    pattern_copy.start()
    for step in range(loads - 1):
        fine_copy(step).start()
    weight_copies[0].start()
    fine_copy(loads - 1).start()
    for copy in weight_copies[1:]:
        copy.start()

    def group_peer(apart):
        return place * near + lax.rem(mine + apart, near)

    def column_peer(apart):
        return lax.rem(place + apart, far) * near + mine

    nexts = lax.rem(me + 1, devices)
    previous = lax.rem(me + devices - 1, devices)
    barrier = pltpu.get_barrier_semaphore()
    peers = [group_peer(a) for a in range(1, near)] + [column_peer(a) for a in range(1, far)] + [nexts, previous]
    for peer in peers:
        pl.semaphore_signal(barrier, inc=1, device_id=(peer,), device_id_type=MESH)

    pattern_copy.wait()
    wide_onehot[...] = wide_rows_onehot(plan, pattern_ref[...], 0)
    for level in plan.narrow:
        onehot[pl.ds(plan.offsets[level], kinds * plan.padded[level]), :] = narrow_onehot(
            plan, pattern_ref[...], level, 0)
    turned = pattern_ref[...].T
    for level in plan.narrow:
        columns = pl.ds(plan.offsets[level], kinds * plan.padded[level])
        spread_ref[:, columns] = narrow_onehot(plan, turned, level, 1)
    spread_ref[:, pl.ds(plan.narrow_rows, plan.wide_rows)] = wide_rows_onehot(plan, turned, 1)

    def extract(step):
        for row in range(plan.wide_used):
            rows[row, pl.ds(step * load, load), :] = few[step % 2, pl.ds(row, load, stride=PITCH), :].astype(BF16)

    for step in range(loads):
        fine_copy(step).wait()
        for first in range(0, load, 2):
            at = step * load + first
            both = jnp.concatenate([fine_ref[at], fine_ref[at + 1]], axis=1)
            both = jnp.dot(wide_onehot[...], both, preferred_element_type=F32)
            few[step % 2, pl.ds(first * PITCH, plan.wide_rows), :] = both[:, :width]
            few[step % 2, pl.ds((first + 1) * PITCH, plan.wide_rows), :] = both[:, width:]
        if step > 0:
            extract(step - 1)
    extract(loads - 1)
    weight_copies[0].wait()
    for position, level in enumerate(plan.wide):
        first = position * kinds
        joined = jnp.concatenate([rows[first + kind] for kind in range(kinds)], axis=1)
        coarse = jnp.dot(joined, restrict_ref[level], preferred_element_type=F32)
        coarse_ref[position] = (coarse * plan.spans[level] ** (-0.5)).astype(BF16)
    base = len(plan.wide) * kinds
    halo_ref[0] = rows[base]
    halo_ref[1] = rows[base + 1]

    pl.semaphore_wait(barrier, len(peers))

    def part_of(index):
        return pl.ds(pl.multiple_of(index * part, part), part)

    copies = []
    for apart in range(1, near):
        theirs = lax.rem(mine + apart, near)
        copies.append(pltpu.make_async_remote_copy(
            src_ref=coarse_ref.at[pl.ds(local, crossing), part_of(theirs), :],
            dst_ref=from_group.at[apart],
            send_sem=group_send.at[apart], recv_sem=group_recv.at[apart],
            device_id=(group_peer(apart),), device_id_type=MESH))
    halo_copies = []
    for side, peer in ((0, previous), (1, nexts)):
        halo_copies.append(pltpu.make_async_remote_copy(
            src_ref=halo_ref.at[side], dst_ref=beside_ref.at[1 - side],
            send_sem=halo_send.at[side], recv_sem=halo_recv.at[1 - side],
            device_id=(peer,), device_id_type=MESH))
    for copy in copies + halo_copies:
        copy.start()

    for copy in weight_copies[1:]:
        copy.wait()
    for position, level in enumerate(plan.narrow):
        half = jnp.dot(restrict_ref[level], inverse_ref[level], preferred_element_type=F32).astype(BF16)
        full = lax.dot_general(half, restrict_ref[level], (((1,), (1,)), ((), ())), preferred_element_type=F32)
        joint[position] = (full * plan.spans[level] ** (-0.5)).astype(BF16)

    edge = lax.broadcasted_iota(jnp.int32, (blocks, width), 0)

    def narrow(step, _):
        here = chunk_of(step)
        stencils = jnp.concatenate([stencil_ref[0], stencil_ref[1], stencil_ref[2]], axis=1)
        for first in range(0, chunk, 2):
            at = step * chunk + first
            both = jnp.concatenate([fine_ref[at], fine_ref[at + 1]], axis=1)
            both = jnp.dot(onehot[...], both, preferred_element_type=F32).astype(BF16)
            grouped[first] = both[:, :width]
            grouped[first + 1] = both[:, width:]
        for slot in range(chunk):
            at = step * chunk + slot
            three = jnp.dot(fine_ref[at], stencils, preferred_element_type=F32)
            earlier = jnp.where(edge == 0, 0.0, pltpu.roll(three[:, :width], 1, 0))
            later = jnp.where(edge == blocks - 1, 0.0, pltpu.roll(three[:, 2 * width :], blocks - 1, 0))
            level0_ref[at] = three[:, width : 2 * width] + earlier + later
        for position, level in enumerate(plan.narrow):
            padded = plan.padded[level]
            slices = [pl.ds(plan.offsets[level] + kind * padded, padded) for kind in range(kinds)]
            joined = jnp.concatenate(
                [grouped[:, tile, :].reshape(chunk * padded, width) for tile in slices], axis=1)
            lifted = jnp.dot(joined, joint[position], preferred_element_type=F32).astype(BF16)
            for kind, tile in enumerate(slices):
                table_ref[here, tile, :] = lifted[:, kind * width : (kind + 1) * width].reshape(chunk, padded, width)
        return 0

    def lift_wide(position, rounded):
        level = plan.wide[position]
        solved = jnp.dot(rounded, inverse_ref[level], preferred_element_type=F32).astype(BF16)
        lifted = lax.dot_general(
            solved, restrict_ref[level], (((1,), (1,)), ((), ())), preferred_element_type=F32)
        for kind in range(kinds):
            wide_f32[pl.ds(position * kinds + kind, plan.vectors, stride=PITCH), :] = (
                lifted[:, kind * width : (kind + 1) * width])

    first_stop = steps // 4
    second_stop = steps // 2
    lax.fori_loop(0, first_stop, narrow, 0)

    total = coarse_ref[pl.ds(local, crossing), part_of(mine), :].astype(F32)
    for apart, copy in enumerate(copies, 1):
        copy.wait_recv()
        total = total + from_group[apart].astype(F32)
    to_column[...] = total.astype(BF16)

    column_copies = []
    for apart in range(1, far):
        column_copies.append(pltpu.make_async_remote_copy(
            src_ref=to_column.at[pl.ds(1, crossing - 1)], dst_ref=from_column.at[apart],
            send_sem=column_send.at[apart], recv_sem=column_recv.at[apart],
            device_id=(column_peer(apart),), device_id_type=MESH))
    for copy in column_copies:
        copy.start()

    for copy in halo_copies:
        copy.wait_recv()
    for row in range(plan.wide_used, plan.wide_rows):
        wide_f32[pl.ds(row, plan.vectors, stride=PITCH), :] = jnp.zeros((plan.vectors, width), F32)
    wide_f32[pl.ds(base, plan.vectors, stride=PITCH), :] = jnp.dot(beside_ref[0], stencil_ref[0], preferred_element_type=F32)
    wide_f32[pl.ds(base + 1, plan.vectors, stride=PITCH), :] = jnp.dot(beside_ref[1], stencil_ref[2], preferred_element_type=F32)
    for position in range(local):
        lift_wide(position, coarse_ref[position])
    lax.fori_loop(first_stop, second_stop, narrow, 0)

    to_group[0] = to_column[0]
    sums = [to_column[index].astype(F32) for index in range(crossing)]
    for apart, copy in enumerate(column_copies, 1):
        copy.wait_recv()
        source = lax.rem(place + far - apart, far)
        for index in range(1, crossing):
            reach = plan.groups[plan.crossing[index]] // near
            keep = (source // reach == place // reach).astype(F32)
            sums[index] = sums[index] + keep * from_column[apart, index - 1].astype(F32)
    for index in range(1, crossing):
        to_group[index] = sums[index].astype(BF16)

    back_copies = []
    for apart in range(1, near):
        back_copies.append(pltpu.make_async_remote_copy(
            src_ref=to_group, dst_ref=back.at[apart],
            send_sem=back_send.at[apart], recv_sem=back_recv.at[apart],
            device_id=(group_peer(apart),), device_id_type=MESH))
    for copy in back_copies:
        copy.start()

    lax.fori_loop(second_stop, steps, narrow, 0)
    for copy in copies:
        copy.wait_send()
    coarse_ref[pl.ds(local, crossing), part_of(mine), :] = to_group[...]
    for apart, copy in enumerate(back_copies, 1):
        copy.wait_recv()
        source = lax.rem(mine + near - apart, near)
        coarse_ref[pl.ds(local, crossing), part_of(source), :] = back[apart]
    for position in range(local, len(plan.wide)):
        lift_wide(position, coarse_ref[position])
    for vector in range(plan.vectors):
        table_ref[vector, pl.ds(plan.narrow_rows, plan.wide_rows), :] = (
            wide_f32[pl.ds(vector * PITCH, plan.wide_rows), :].astype(BF16))
    for copy in halo_copies + column_copies + back_copies:
        copy.wait_send()


def final_kernel(plan, pieces, spread_ref, table_ref, level0_ref, out_hbm, staged, out_sem):
    width = plan.width
    copies, at = [], 0
    for index, piece in enumerate(pieces):
        for first in range(at, at + piece, 2):
            tables = jnp.concatenate([table_ref[first], table_ref[first + 1]], axis=1)
            both = jnp.dot(spread_ref[...], tables, preferred_element_type=F32)
            staged[first] = both[:, :width] + level0_ref[first]
            staged[first + 1] = both[:, width:] + level0_ref[first + 1]
        here = pl.ds(at, piece)
        copy = pltpu.make_async_copy(staged.at[here], out_hbm.at[here], out_sem.at[index])
        copy.start()
        copies.append(copy)
        at += piece
    for copy in copies:
        copy.wait()


def shards(fine, pattern, stencil, restrict, coarse_inv):
    devices = lax.axis_size("gx")
    vectors, blocks, width = fine.shape
    levels, kinds = restrict.shape[:2]
    plan = Plan(devices, vectors, blocks, width, levels, kinds)
    stacked = restrict.reshape(levels, kinds * width, width)
    wide_count = len(plan.wide)
    chunk = 16
    near = plan.groups[plan.crossing[0]]
    far = devices // near
    crossing = len(plan.crossing)
    part = vectors // near
    table_rows = plan.narrow_rows + plan.wide_rows
    vmem = pl.BlockSpec(memory_space=pltpu.VMEM)
    hbm = pl.BlockSpec(memory_space=pltpu.HBM)
    dma = pltpu.SemaphoreType.DMA
    pinned = [pltpu.with_memory_space_constraint(x, pltpu.HBM) for x in (pattern, fine, stacked, coarse_inv, stencil)]
    table, level0, spread = pl.pallas_call(
        functools.partial(exchange_kernel, plan, chunk),
        out_shape=(
            pltpu.VMEM((vectors, table_rows, width), BF16),
            pltpu.VMEM((vectors, blocks, width), F32),
            pltpu.VMEM((blocks, table_rows), BF16),
        ),
        in_specs=[hbm] * 5,
        out_specs=(vmem, vmem, vmem),
        scratch_shapes=[
            pltpu.VMEM(pattern.shape, jnp.int32),
            pltpu.VMEM(fine.shape, BF16),
            pltpu.VMEM(stacked.shape, BF16),
            pltpu.VMEM(coarse_inv.shape, BF16),
            pltpu.VMEM(stencil.shape, BF16),
            pltpu.VMEM((vectors * PITCH, width), F32),
            pltpu.VMEM((plan.wide_rows, blocks), BF16),
            pltpu.VMEM((plan.narrow_rows, blocks), BF16),
            pltpu.VMEM((2, 16 * PITCH, width), F32),
            pltpu.VMEM((chunk, plan.narrow_rows, width), BF16),
            pltpu.VMEM((len(plan.narrow), kinds * width, kinds * width), BF16),
            pltpu.VMEM((plan.wide_used, vectors, width), BF16),
            pltpu.VMEM((wide_count, vectors, width), BF16),
            pltpu.VMEM((2, vectors, width), BF16),
            pltpu.VMEM((2, vectors, width), BF16),
            pltpu.VMEM((near, crossing, part, width), BF16),
            pltpu.VMEM((crossing, part, width), BF16),
            pltpu.VMEM((far, crossing - 1, part, width), BF16),
            pltpu.VMEM((crossing, part, width), BF16),
            pltpu.VMEM((near, crossing, part, width), BF16),
            dma((vectors // 16,)), dma((5,)),
            dma((near,)), dma((near,)), dma((far,)), dma((far,)), dma((near,)), dma((near,)), dma((2,)), dma((2,)),
        ],
        compiler_params=pltpu.CompilerParams(
            collective_id=0, has_side_effects=True, vmem_limit_bytes=VMEM_LIMIT),
        name="exchange",
    )(*pinned)

    pieces = [8] * (vectors // 8 - 1) + [4, 2, 2]
    return pl.pallas_call(
        functools.partial(final_kernel, plan, pieces),
        out_shape=jax.ShapeDtypeStruct(fine.shape, F32),
        in_specs=[vmem, vmem, vmem],
        out_specs=pl.BlockSpec(memory_space=pl.ANY),
        scratch_shapes=[pltpu.VMEM(fine.shape, F32), dma((len(pieces),))],
        compiler_params=pltpu.CompilerParams(vmem_limit_bytes=VMEM_LIMIT),
        name="final",
    )(spread, table, level0)


def solution(mesh):
    in_specs = (P(None, "gx", None), P(None, "gx"), P(), P(), P())
    out_specs = P(None, "gx", None)
    return jax.shard_map(shards, mesh=mesh, in_specs=in_specs, out_specs=out_specs, check_vma=False)
```

```python
import functools

import jax
import jax.numpy as jnp
from jax import lax
from jax.experimental import pallas as pl
from jax.experimental.pallas import tpu as pltpu
from jax.sharding import PartitionSpec as P

MESH = pl.DeviceIdType.MESH
F32 = jnp.float32
BF16 = jnp.bfloat16
TILE = 16
VMEM_LIMIT = 30 * 2**20


def round_up(value, unit):
    return -(-value // unit) * unit


class Plan:
    def __init__(self, devices, vectors, blocks, width, levels, kinds):
        self.devices, self.vectors, self.blocks = devices, vectors, blocks
        self.width, self.levels, self.kinds = width, levels, kinds
        all_blocks = devices * blocks
        self.spans, self.local_spans, self.counts, self.groups = [], [], [], []
        for level in range(levels):
            span = all_blocks // max(all_blocks // 4 ** (level + 1), 1)
            local = min(span, blocks)
            self.spans.append(span)
            self.local_spans.append(local)
            self.counts.append(blocks // local)
            self.groups.append(span // local)
        self.narrow = [l for l in range(levels) if self.counts[l] > 1]
        self.wide = [l for l in range(levels) if self.counts[l] == 1]
        self.crossing = [l for l in range(levels) if self.groups[l] > 1]
        self.padded = {l: round_up(self.counts[l], TILE) for l in self.narrow}
        self.offsets, at = {}, 0
        for l in self.narrow:
            self.offsets[l] = at
            at += kinds * self.padded[l]
        self.narrow_rows = at
        self.wide_used = len(self.wide) * kinds + 2
        self.wide_rows = round_up(self.wide_used, TILE)


def wide_rows_onehot(plan, pattern, rows_axis):
    shape = (plan.wide_rows, plan.blocks) if rows_axis == 0 else (plan.blocks, plan.wide_rows)
    row = lax.broadcasted_iota(jnp.int32, shape, rows_axis)
    block = lax.broadcasted_iota(jnp.int32, shape, 1 - rows_axis)
    base = len(plan.wide) * plan.kinds
    hit = ((row == base) & (block == 0)) | ((row == base + 1) & (block == plan.blocks - 1))
    for position, level in enumerate(plan.wide):
        kinds = pattern[level : level + 1, :] if rows_axis == 0 else pattern[:, level : level + 1]
        first = position * plan.kinds
        inside = (row >= first) & (row < first + plan.kinds)
        hit = hit | (inside & (row - first == kinds))
    return hit.astype(F32).astype(BF16)


def narrow_onehot(plan, pattern, level, rows_axis):
    padded = plan.padded[level]
    rows = plan.kinds * padded
    shape = (rows, plan.blocks) if rows_axis == 0 else (plan.blocks, rows)
    row = lax.broadcasted_iota(jnp.int32, shape, rows_axis)
    block = lax.broadcasted_iota(jnp.int32, shape, 1 - rows_axis)
    kinds = pattern[level : level + 1, :] if rows_axis == 0 else pattern[:, level : level + 1]
    target = kinds * padded + block // plan.local_spans[level]
    return (row == target).astype(F32).astype(BF16)

PITCH = 40


def exchange_kernel(plan, segments, pattern_hbm, fine_hbm, restrict_hbm, inverse_hbm, stencil_hbm,
                    table_ref, level0_ref, spread_ref,
                    pattern_ref, fine_ref, restrict_ref, inverse_ref, stencil_ref, wide_f32, wide_onehot, onehot, few,
                    grouped, joint, pair_weights, split, rows, coarse_ref, halo_ref, beside_ref,
                    from_group, to_column, from_column, to_group, back,
                    fine_sem, weight_sem, group_send, group_recv,
                    column_send, column_recv, back_send, back_recv, halo_send, halo_recv):
    width, kinds, blocks = plan.width, plan.kinds, plan.blocks
    load = 16
    loads = plan.vectors // load
    devices = plan.devices
    near = plan.groups[plan.crossing[0]]
    far = devices // near
    local = len(plan.wide) - len(plan.crossing)
    crossing = len(plan.crossing)
    part = plan.vectors // near
    me = lax.axis_index("gx")
    mine = lax.rem(me, near)
    place = me // near

    def fine_copy(step):
        here = pl.ds(step * load, load)
        return pltpu.make_async_copy(fine_hbm.at[here], fine_ref.at[here], fine_sem.at[step])

    wide_first = plan.wide[0]
    wide_weights = pl.ds(wide_first, len(plan.wide))
    weight_copies = [
        pltpu.make_async_copy(restrict_hbm.at[wide_weights], restrict_ref.at[wide_weights], weight_sem.at[0]),
        pltpu.make_async_copy(restrict_hbm.at[pl.ds(0, wide_first)], restrict_ref.at[pl.ds(0, wide_first)], weight_sem.at[1]),
        pltpu.make_async_copy(inverse_hbm, inverse_ref, weight_sem.at[2]),
        pltpu.make_async_copy(stencil_hbm, stencil_ref, weight_sem.at[3]),
    ]
    pattern_copy = pltpu.make_async_copy(pattern_hbm, pattern_ref, weight_sem.at[4])
    pattern_copy.start()
    for step in range(loads - 1):
        fine_copy(step).start()
    weight_copies[0].start()
    fine_copy(loads - 1).start()
    for copy in weight_copies[1:]:
        copy.start()

    def group_peer(apart):
        return place * near + lax.rem(mine + apart, near)

    def column_peer(apart):
        return lax.rem(place + apart, far) * near + mine

    nexts = lax.rem(me + 1, devices)
    previous = lax.rem(me + devices - 1, devices)
    barrier = pltpu.get_barrier_semaphore()
    peers = [group_peer(a) for a in range(1, near)] + [column_peer(a) for a in range(1, far)] + [nexts, previous]
    for peer in peers:
        pl.semaphore_signal(barrier, inc=1, device_id=(peer,), device_id_type=MESH)

    pattern_copy.wait()
    wide_onehot[...] = wide_rows_onehot(plan, pattern_ref[...], 0)
    for level in plan.narrow:
        onehot[pl.ds(plan.offsets[level], kinds * plan.padded[level]), :] = narrow_onehot(
            plan, pattern_ref[...], level, 0)
    turned = pattern_ref[...].T
    for level in plan.narrow:
        columns = pl.ds(plan.offsets[level], kinds * plan.padded[level])
        spread_ref[:, columns] = narrow_onehot(plan, turned, level, 1)
    spread_ref[:, pl.ds(plan.narrow_rows, plan.wide_rows)] = wide_rows_onehot(plan, turned, 1)

    def extract(step):
        for row in range(plan.wide_used):
            rows[row, pl.ds(step * load, load), :] = few[step % 2, pl.ds(row, load, stride=PITCH), :].astype(BF16)

    for step in range(loads):
        fine_copy(step).wait()
        for first in range(0, load, 2):
            at = step * load + first
            both = jnp.concatenate([fine_ref[at], fine_ref[at + 1]], axis=1)
            both = jnp.dot(wide_onehot[...], both, preferred_element_type=F32)
            few[step % 2, pl.ds(first * PITCH, plan.wide_rows), :] = both[:, :width]
            few[step % 2, pl.ds((first + 1) * PITCH, plan.wide_rows), :] = both[:, width:]
        if step > 0:
            extract(step - 1)
    extract(loads - 1)
    weight_copies[0].wait()
    for position, level in enumerate(plan.wide):
        first = position * kinds
        joined = jnp.concatenate([rows[first + kind] for kind in range(kinds)], axis=1)
        coarse = jnp.dot(joined, restrict_ref[level], preferred_element_type=F32)
        coarse_ref[position] = (coarse * plan.spans[level] ** (-0.5)).astype(BF16)
    base = len(plan.wide) * kinds
    halo_ref[0] = rows[base]
    halo_ref[1] = rows[base + 1]

    pl.semaphore_wait(barrier, len(peers))

    def part_of(index):
        return pl.ds(pl.multiple_of(index * part, part), part)

    copies = []
    for apart in range(1, near):
        theirs = lax.rem(mine + apart, near)
        copies.append(pltpu.make_async_remote_copy(
            src_ref=coarse_ref.at[pl.ds(local, crossing), part_of(theirs), :],
            dst_ref=from_group.at[apart],
            send_sem=group_send.at[apart], recv_sem=group_recv.at[apart],
            device_id=(group_peer(apart),), device_id_type=MESH))
    halo_copies = []
    for side, peer in ((0, previous), (1, nexts)):
        halo_copies.append(pltpu.make_async_remote_copy(
            src_ref=halo_ref.at[side], dst_ref=beside_ref.at[1 - side],
            send_sem=halo_send.at[side], recv_sem=halo_recv.at[1 - side],
            device_id=(peer,), device_id_type=MESH))
    for copy in copies + halo_copies:
        copy.start()

    for copy in weight_copies[1:]:
        copy.wait()
    for position, level in enumerate(plan.narrow):
        half = jnp.dot(restrict_ref[level], inverse_ref[level], preferred_element_type=F32).astype(BF16)
        full = lax.dot_general(half, restrict_ref[level], (((1,), (1,)), ((), ())), preferred_element_type=F32)
        joint[position] = (full * plan.spans[level] ** (-0.5)).astype(BF16)

    none = jnp.zeros((width, width), BF16)
    pair_weights[...] = jnp.concatenate([
        jnp.concatenate([stencil_ref[1], stencil_ref[0], none, stencil_ref[2]], axis=1),
        jnp.concatenate([stencil_ref[2], stencil_ref[1], stencil_ref[0], none], axis=1)], axis=0)
    pairs = blocks // 2
    edge = lax.broadcasted_iota(jnp.int32, (pairs, width), 0)
    ahead = (edge > 0).astype(F32)
    behind = (edge < pairs - 1).astype(F32)

    def narrow(start, chunk):
        for slot in range(0, chunk, 2):
            at = start + slot
            both = jnp.concatenate([fine_ref[at], fine_ref[at + 1]], axis=1)
            both = jnp.dot(onehot[...], both, preferred_element_type=F32).astype(BF16)
            grouped[slot] = both[:, :width]
            grouped[slot + 1] = both[:, width:]
        for slot in range(chunk):
            at = start + slot
            turn = slot % 4
            split[turn] = fine_ref[at].astype(F32)
            evens = split[turn, pl.ds(0, pairs, stride=2), :].astype(BF16)
            odds = split[turn, pl.ds(1, pairs, stride=2), :].astype(BF16)
            four = jnp.dot(jnp.concatenate([evens, odds], axis=1), pair_weights[...], preferred_element_type=F32)
            earlier = pltpu.roll(four[:, 2 * width : 3 * width], 1, 0) * ahead
            later = pltpu.roll(four[:, 3 * width :], pairs - 1, 0) * behind
            level0_ref[at, pl.ds(0, pairs, stride=2), :] = four[:, :width] + earlier
            level0_ref[at, pl.ds(1, pairs, stride=2), :] = four[:, width : 2 * width] + later
        for position, level in enumerate(plan.narrow):
            padded = plan.padded[level]
            slices = [pl.ds(plan.offsets[level] + kind * padded, padded) for kind in range(kinds)]
            joined = jnp.concatenate(
                [grouped[pl.ds(0, chunk), tile, :].reshape(chunk * padded, width) for tile in slices], axis=1)
            lifted = jnp.dot(joined, joint[position], preferred_element_type=F32).astype(BF16)
            for kind, tile in enumerate(slices):
                table_ref[pl.ds(start, chunk), tile, :] = (
                    lifted[:, kind * width : (kind + 1) * width].reshape(chunk, padded, width))

    def lift_wide(position, rounded):
        level = plan.wide[position]
        solved = jnp.dot(rounded, inverse_ref[level], preferred_element_type=F32).astype(BF16)
        lifted = lax.dot_general(
            solved, restrict_ref[level], (((1,), (1,)), ((), ())), preferred_element_type=F32)
        for kind in range(kinds):
            wide_f32[pl.ds(position * kinds + kind, plan.vectors, stride=PITCH), :] = (
                lifted[:, kind * width : (kind + 1) * width])

    starts = [sum(segments[:index]) for index in range(len(segments))]
    narrow(starts[0], segments[0])

    total = coarse_ref[pl.ds(local, crossing), part_of(mine), :].astype(F32)
    for apart, copy in enumerate(copies, 1):
        copy.wait_recv()
        total = total + from_group[apart].astype(F32)
    to_column[...] = total.astype(BF16)

    column_copies = []
    for apart in range(1, far):
        column_copies.append(pltpu.make_async_remote_copy(
            src_ref=to_column.at[pl.ds(1, crossing - 1)], dst_ref=from_column.at[apart],
            send_sem=column_send.at[apart], recv_sem=column_recv.at[apart],
            device_id=(column_peer(apart),), device_id_type=MESH))
    for copy in column_copies:
        copy.start()

    for copy in halo_copies:
        copy.wait_recv()
    for row in range(plan.wide_used, plan.wide_rows):
        wide_f32[pl.ds(row, plan.vectors, stride=PITCH), :] = jnp.zeros((plan.vectors, width), F32)
    wide_f32[pl.ds(base, plan.vectors, stride=PITCH), :] = jnp.dot(beside_ref[0], stencil_ref[0], preferred_element_type=F32)
    wide_f32[pl.ds(base + 1, plan.vectors, stride=PITCH), :] = jnp.dot(beside_ref[1], stencil_ref[2], preferred_element_type=F32)
    for position in range(local):
        lift_wide(position, coarse_ref[position])
    narrow(starts[1], segments[1])

    to_group[0] = to_column[0]
    sums = [to_column[index].astype(F32) for index in range(crossing)]
    for apart, copy in enumerate(column_copies, 1):
        copy.wait_recv()
        source = lax.rem(place + far - apart, far)
        for index in range(1, crossing):
            reach = plan.groups[plan.crossing[index]] // near
            keep = (source // reach == place // reach).astype(F32)
            sums[index] = sums[index] + keep * from_column[apart, index - 1].astype(F32)
    for index in range(1, crossing):
        to_group[index] = sums[index].astype(BF16)

    back_copies = []
    for apart in range(1, near):
        back_copies.append(pltpu.make_async_remote_copy(
            src_ref=to_group, dst_ref=back.at[apart],
            send_sem=back_send.at[apart], recv_sem=back_recv.at[apart],
            device_id=(group_peer(apart),), device_id_type=MESH))
    for copy in back_copies:
        copy.start()

    narrow(starts[2], segments[2])
    for copy in copies:
        copy.wait_send()
    coarse_ref[pl.ds(local, crossing), part_of(mine), :] = to_group[...]
    for apart, copy in enumerate(back_copies, 1):
        copy.wait_recv()
        source = lax.rem(mine + near - apart, near)
        coarse_ref[pl.ds(local, crossing), part_of(source), :] = back[apart]
    for position in range(local, len(plan.wide)):
        lift_wide(position, coarse_ref[position])
    for vector in range(plan.vectors):
        table_ref[vector, pl.ds(plan.narrow_rows, plan.wide_rows), :] = (
            wide_f32[pl.ds(vector * PITCH, plan.wide_rows), :].astype(BF16))
    for copy in halo_copies + column_copies + back_copies:
        copy.wait_send()


def final_kernel(plan, pieces, spread_ref, table_ref, level0_ref, out_hbm, staged, out_sem):
    width = plan.width
    copies, at = [], 0
    for index, piece in enumerate(pieces):
        for first in range(at, at + piece, 2):
            tables = jnp.concatenate([table_ref[first], table_ref[first + 1]], axis=1)
            both = jnp.dot(spread_ref[...], tables, preferred_element_type=F32)
            staged[first] = both[:, :width] + level0_ref[first]
            staged[first + 1] = both[:, width:] + level0_ref[first + 1]
        here = pl.ds(at, piece)
        copy = pltpu.make_async_copy(staged.at[here], out_hbm.at[here], out_sem.at[index])
        copy.start()
        copies.append(copy)
        at += piece
    for copy in copies:
        copy.wait()


def shards(fine, pattern, stencil, restrict, coarse_inv):
    devices = lax.axis_size("gx")
    vectors, blocks, width = fine.shape
    levels, kinds = restrict.shape[:2]
    plan = Plan(devices, vectors, blocks, width, levels, kinds)
    stacked = restrict.reshape(levels, kinds * width, width)
    wide_count = len(plan.wide)
    some = vectors // 4
    segments = (some, 2 * some, vectors - 3 * some)
    near = plan.groups[plan.crossing[0]]
    far = devices // near
    crossing = len(plan.crossing)
    part = vectors // near
    table_rows = plan.narrow_rows + plan.wide_rows
    vmem = pl.BlockSpec(memory_space=pltpu.VMEM)
    hbm = pl.BlockSpec(memory_space=pltpu.HBM)
    dma = pltpu.SemaphoreType.DMA
    pinned = [pltpu.with_memory_space_constraint(x, pltpu.HBM) for x in (pattern, fine, stacked, coarse_inv, stencil)]
    table, level0, spread = pl.pallas_call(
        functools.partial(exchange_kernel, plan, segments),
        out_shape=(
            pltpu.VMEM((vectors, table_rows, width), BF16),
            pltpu.VMEM((vectors, blocks, width), F32),
            pltpu.VMEM((blocks, table_rows), BF16),
        ),
        in_specs=[hbm] * 5,
        out_specs=(vmem, vmem, vmem),
        scratch_shapes=[
            pltpu.VMEM(pattern.shape, jnp.int32),
            pltpu.VMEM(fine.shape, BF16),
            pltpu.VMEM(stacked.shape, BF16),
            pltpu.VMEM(coarse_inv.shape, BF16),
            pltpu.VMEM(stencil.shape, BF16),
            pltpu.VMEM((vectors * PITCH, width), F32),
            pltpu.VMEM((plan.wide_rows, blocks), BF16),
            pltpu.VMEM((plan.narrow_rows, blocks), BF16),
            pltpu.VMEM((2, 16 * PITCH, width), F32),
            pltpu.VMEM((max(segments), plan.narrow_rows, width), BF16),
            pltpu.VMEM((len(plan.narrow), kinds * width, kinds * width), BF16),
            pltpu.VMEM((2 * width, 4 * width), BF16),
            pltpu.VMEM((4, blocks, width), F32),
            pltpu.VMEM((plan.wide_used, vectors, width), BF16),
            pltpu.VMEM((wide_count, vectors, width), BF16),
            pltpu.VMEM((2, vectors, width), BF16),
            pltpu.VMEM((2, vectors, width), BF16),
            pltpu.VMEM((near, crossing, part, width), BF16),
            pltpu.VMEM((crossing, part, width), BF16),
            pltpu.VMEM((far, crossing - 1, part, width), BF16),
            pltpu.VMEM((crossing, part, width), BF16),
            pltpu.VMEM((near, crossing, part, width), BF16),
            dma((vectors // 16,)), dma((5,)),
            dma((near,)), dma((near,)), dma((far,)), dma((far,)), dma((near,)), dma((near,)), dma((2,)), dma((2,)),
        ],
        compiler_params=pltpu.CompilerParams(
            collective_id=0, has_side_effects=True, vmem_limit_bytes=VMEM_LIMIT),
        name="exchange",
    )(*pinned)

    pieces = [2, 2, 4] + [8] * (vectors // 8 - 2) + [4, 2, 2]
    return pl.pallas_call(
        functools.partial(final_kernel, plan, pieces),
        out_shape=jax.ShapeDtypeStruct(fine.shape, F32),
        in_specs=[vmem, vmem, vmem],
        out_specs=pl.BlockSpec(memory_space=pl.ANY),
        scratch_shapes=[pltpu.VMEM(fine.shape, F32), dma((len(pieces),))],
        compiler_params=pltpu.CompilerParams(vmem_limit_bytes=VMEM_LIMIT),
        name="final",
    )(spread, table, level0)


def solution(mesh):
    in_specs = (P(None, "gx", None), P(None, "gx"), P(), P(), P())
    out_specs = P(None, "gx", None)
    return jax.shard_map(shards, mesh=mesh, in_specs=in_specs, out_specs=out_specs, check_vma=False)
```

```python
import functools

import jax
import jax.numpy as jnp
from jax import lax
from jax.experimental import pallas as pl
from jax.experimental.pallas import tpu as pltpu
from jax.sharding import PartitionSpec as P

MESH = pl.DeviceIdType.MESH
F32 = jnp.float32
BF16 = jnp.bfloat16
TILE = 16
VMEM_LIMIT = 30 * 2**20


def round_up(value, unit):
    return -(-value // unit) * unit


class Plan:
    def __init__(self, devices, vectors, blocks, width, levels, kinds):
        self.devices, self.vectors, self.blocks = devices, vectors, blocks
        self.width, self.levels, self.kinds = width, levels, kinds
        all_blocks = devices * blocks
        self.spans, self.local_spans, self.counts, self.groups = [], [], [], []
        for level in range(levels):
            span = all_blocks // max(all_blocks // 4 ** (level + 1), 1)
            local = min(span, blocks)
            self.spans.append(span)
            self.local_spans.append(local)
            self.counts.append(blocks // local)
            self.groups.append(span // local)
        self.narrow = [l for l in range(levels) if self.counts[l] > 1]
        self.wide = [l for l in range(levels) if self.counts[l] == 1]
        self.crossing = [l for l in range(levels) if self.groups[l] > 1]
        self.padded = {l: round_up(self.counts[l], TILE // 2) for l in self.narrow}
        self.offsets, at = {}, 0
        for l in self.narrow:
            self.offsets[l] = at
            at += kinds * self.padded[l]
        self.narrow_rows = at
        self.small = [l for l in self.narrow if self.padded[l] % TILE]
        self.cut = min([self.offsets[l] for l in self.small], default=at)
        self.narrow_rows = round_up(at, 2 * TILE)
        self.wide_used = len(self.wide) * kinds + 2
        self.wide_rows = round_up(self.wide_used, TILE)


def wide_rows_onehot(plan, pattern, rows_axis):
    shape = (plan.wide_rows, plan.blocks) if rows_axis == 0 else (plan.blocks, plan.wide_rows)
    row = lax.broadcasted_iota(jnp.int32, shape, rows_axis)
    block = lax.broadcasted_iota(jnp.int32, shape, 1 - rows_axis)
    base = len(plan.wide) * plan.kinds
    hit = ((row == base) & (block == 0)) | ((row == base + 1) & (block == plan.blocks - 1))
    for position, level in enumerate(plan.wide):
        kinds = pattern[level : level + 1, :] if rows_axis == 0 else pattern[:, level : level + 1]
        first = position * plan.kinds
        inside = (row >= first) & (row < first + plan.kinds)
        hit = hit | (inside & (row - first == kinds))
    return hit.astype(F32).astype(BF16)


def narrow_onehot(plan, pattern, level, rows_axis):
    padded = plan.padded[level]
    rows = plan.kinds * padded
    shape = (rows, plan.blocks) if rows_axis == 0 else (plan.blocks, rows)
    row = lax.broadcasted_iota(jnp.int32, shape, rows_axis)
    block = lax.broadcasted_iota(jnp.int32, shape, 1 - rows_axis)
    kinds = pattern[level : level + 1, :] if rows_axis == 0 else pattern[:, level : level + 1]
    target = kinds * padded + block // plan.local_spans[level]
    return (row == target).astype(F32).astype(BF16)

PITCH = 40


def exchange_kernel(plan, segments, pattern_hbm, fine_hbm, restrict_hbm, inverse_hbm, stencil_hbm,
                    table_ref, level0_ref, spread_ref,
                    pattern_ref, fine_ref, restrict_ref, inverse_ref, stencil_ref, wide_f32, wide_onehot, onehot, few,
                    grouped, grouped_small, joint, pair_weights, split, rows, coarse_ref, own_ref, result_ref, halo_ref, beside_ref,
                    from_group, to_column, early_ref, from_column, to_group, back,
                    fine_sem, weight_sem, group_send, group_recv,
                    early_send, early_recv, column_send, column_recv, back_send, back_recv, halo_send, halo_recv):
    width, kinds, blocks = plan.width, plan.kinds, plan.blocks
    devices = plan.devices
    near = plan.groups[plan.crossing[0]]
    far = devices // near
    local = len(plan.wide) - len(plan.crossing)
    crossing = len(plan.crossing)
    part = plan.vectors // near
    me = lax.axis_index("gx")
    early = me < 2
    mine = lax.rem(me, near)
    place = me // near

    def part_of(index):
        return pl.ds(pl.multiple_of(index * part, part), part)

    def part_at(turn):
        return lax.rem(mine + 1 + turn, near)

    def fine_copy(turn):
        here = part_of(part_at(turn))
        return pltpu.make_async_copy(fine_hbm.at[here], fine_ref.at[here], fine_sem.at[turn])

    wide_first = plan.wide[0]
    wide_weights = pl.ds(wide_first, len(plan.wide))
    weight_copies = [
        pltpu.make_async_copy(restrict_hbm.at[wide_weights], restrict_ref.at[wide_weights], weight_sem.at[0]),
        pltpu.make_async_copy(restrict_hbm.at[pl.ds(0, wide_first)], restrict_ref.at[pl.ds(0, wide_first)], weight_sem.at[1]),
        pltpu.make_async_copy(inverse_hbm, inverse_ref, weight_sem.at[2]),
        pltpu.make_async_copy(stencil_hbm, stencil_ref, weight_sem.at[3]),
    ]
    pattern_copy = pltpu.make_async_copy(pattern_hbm, pattern_ref, weight_sem.at[4])
    pattern_copy.start()
    for turn in range(near - 1):
        fine_copy(turn).start()
    weight_copies[0].start()
    fine_copy(near - 1).start()
    for copy in weight_copies[1:]:
        copy.start()

    def group_peer(apart):
        return place * near + lax.rem(mine + apart, near)

    def column_peer(apart):
        return lax.rem(place + apart, far) * near + mine

    nexts = lax.rem(me + 1, devices)
    previous = lax.rem(me + devices - 1, devices)
    barrier = pltpu.get_barrier_semaphore()
    peers = [group_peer(a) for a in range(1, near)] + [column_peer(a) for a in range(1, far)] + [nexts, previous]
    for peer in peers:
        pl.semaphore_signal(barrier, inc=1, device_id=(peer,), device_id_type=MESH)

    pattern_copy.wait()
    wide_onehot[...] = wide_rows_onehot(plan, pattern_ref[...], 0)
    for level in plan.narrow:
        onehot[pl.ds(plan.offsets[level], kinds * plan.padded[level]), :] = narrow_onehot(
            plan, pattern_ref[...], level, 0)
    turned = pattern_ref[...].T
    for level in plan.narrow:
        columns = pl.ds(plan.offsets[level], kinds * plan.padded[level])
        spread_ref[:, columns] = narrow_onehot(plan, turned, level, 1)
    spread_ref[:, pl.ds(plan.narrow_rows, plan.wide_rows)] = wide_rows_onehot(plan, turned, 1)

    for row in range(plan.wide_used):
        rows[row, part_of(mine), :] = jnp.zeros((part, width), BF16)

    def gather(turn):
        fine_copy(turn).wait()
        for first in range(0, part, 2):
            at = part_at(turn) * part + first
            both = jnp.concatenate([fine_ref[at], fine_ref[at + 1]], axis=1)
            both = jnp.dot(wide_onehot[...], both, preferred_element_type=F32)
            few[turn % 2, pl.ds(first * PITCH, plan.wide_rows), :] = both[:, :width]
            few[turn % 2, pl.ds((first + 1) * PITCH, plan.wide_rows), :] = both[:, width:]

    def extract(turn):
        for row in range(plan.wide_used):
            rows[row, part_of(part_at(turn)), :] = few[turn % 2, pl.ds(row, part, stride=PITCH), :].astype(BF16)

    def coarsen(position, vectors):
        level, first = plan.wide[position], position * kinds
        joined = jnp.concatenate([rows[first + kind, vectors, :] for kind in range(kinds)], axis=1)
        coarse = jnp.dot(joined, restrict_ref[level], preferred_element_type=F32)
        return coarse * plan.spans[level] ** (-0.5)

    every = pl.ds(0, plan.vectors)
    for turn in range(near - 1):
        gather(turn)
        if turn > 0:
            extract(turn - 1)
    extract(near - 2)
    weight_copies[0].wait()
    for index in range(crossing):
        coarse_ref[index] = coarsen(local + index, every).astype(BF16)

    pl.semaphore_wait(barrier, len(peers))

    copies = []
    for apart in range(1, near):
        theirs = lax.rem(mine + apart, near)
        copies.append(pltpu.make_async_remote_copy(
            src_ref=coarse_ref.at[:, part_of(theirs), :],
            dst_ref=from_group.at[apart],
            send_sem=group_send.at[apart], recv_sem=group_recv.at[apart],
            device_id=(group_peer(apart),), device_id_type=MESH))
    for copy in copies:
        copy.start()

    gather(near - 1)
    extract(near - 1)
    for index in range(crossing):
        own_ref[index] = coarsen(local + index, part_of(mine))
    base = len(plan.wide) * kinds
    halo_ref[0] = rows[base]
    halo_ref[1] = rows[base + 1]
    halo_copies = []
    for side, peer in ((0, previous), (1, nexts)):
        halo_copies.append(pltpu.make_async_remote_copy(
            src_ref=halo_ref.at[side], dst_ref=beside_ref.at[1 - side],
            send_sem=halo_send.at[side], recv_sem=halo_recv.at[1 - side],
            device_id=(peer,), device_id_type=MESH))
    for copy in halo_copies:
        copy.start()

    for copy in weight_copies[1:]:
        copy.wait()
    for position, level in enumerate(plan.narrow):
        half = jnp.dot(restrict_ref[level], inverse_ref[level], preferred_element_type=F32).astype(BF16)
        full = lax.dot_general(half, restrict_ref[level], (((1,), (1,)), ((), ())), preferred_element_type=F32)
        joint[position] = (full * plan.spans[level] ** (-0.5)).astype(BF16)

    none = jnp.zeros((width, width), BF16)
    pair_weights[...] = jnp.concatenate([
        jnp.concatenate([stencil_ref[1], stencil_ref[0], none, stencil_ref[2]], axis=1),
        jnp.concatenate([stencil_ref[2], stencil_ref[1], stencil_ref[0], none], axis=1)], axis=0)
    pairs = blocks // 2
    edge = lax.broadcasted_iota(jnp.int32, (pairs, width), 0)
    ahead = (edge > 0).astype(F32)
    behind = (edge < pairs - 1).astype(F32)

    def narrow(start, chunk):
        for slot in range(0, chunk, 2):
            at = start + slot
            both = jnp.concatenate([fine_ref[at], fine_ref[at + 1]], axis=1)
            both = jnp.dot(onehot[...], both, preferred_element_type=F32)
            large = both[: plan.cut].astype(BF16)
            grouped[slot] = large[:, :width]
            grouped[slot + 1] = large[:, width:]
            grouped_small[slot] = both[plan.cut :, :width]
            grouped_small[slot + 1] = both[plan.cut :, width:]
        for slot in range(chunk):
            at = start + slot
            turn = slot % 4
            split[turn] = fine_ref[at].astype(F32)
            evens = split[turn, pl.ds(0, pairs, stride=2), :].astype(BF16)
            odds = split[turn, pl.ds(1, pairs, stride=2), :].astype(BF16)
            four = jnp.dot(jnp.concatenate([evens, odds], axis=1), pair_weights[...], preferred_element_type=F32)
            earlier = pltpu.roll(four[:, 2 * width : 3 * width], 1, 0) * ahead
            later = pltpu.roll(four[:, 3 * width :], pairs - 1, 0) * behind
            level0_ref[at, pl.ds(0, pairs, stride=2), :] = four[:, :width] + earlier
            level0_ref[at, pl.ds(1, pairs, stride=2), :] = four[:, width : 2 * width] + later
        for position, level in enumerate(plan.narrow):
            padded = plan.padded[level]
            small = level in plan.small
            source, first = (grouped_small, plan.cut) if small else (grouped, 0)
            slices = [pl.ds(plan.offsets[level] - first + kind * padded, padded) for kind in range(kinds)]
            joined = jnp.concatenate(
                [source[pl.ds(0, chunk), tile, :].reshape(chunk * padded, width).astype(BF16) for tile in slices], axis=1)
            lifted = jnp.dot(joined, joint[position], preferred_element_type=F32)
            tiles = [lifted[:, kind * width : (kind + 1) * width].reshape(chunk, padded, width) for kind in range(kinds)]
            target = pl.ds(plan.offsets[level], kinds * padded)
            table_ref[pl.ds(start, chunk), target, :] = jnp.concatenate(tiles, axis=1).astype(BF16)

    def lift_wide(position, rounded):
        level = plan.wide[position]
        solved = jnp.dot(rounded, inverse_ref[level], preferred_element_type=F32).astype(BF16)
        lifted = lax.dot_general(
            solved, restrict_ref[level], (((1,), (1,)), ((), ())), preferred_element_type=F32)
        for kind in range(kinds):
            wide_f32[pl.ds(position * kinds + kind, plan.vectors, stride=PITCH), :] = (
                lifted[:, kind * width : (kind + 1) * width])

    starts = [sum(segments[:index]) for index in range(len(segments))]
    narrow(starts[0], segments[0])

    @pl.when(early)
    def _():
        narrow(starts[1], segments[1])


    total = own_ref[...]
    for apart, copy in enumerate(copies, 1):
        copy.wait_recv()
        total = total + from_group[apart].astype(F32)
    to_column[...] = total.astype(BF16)

    column_copies = []
    for apart in range(1, far):
        column_copies.append(pltpu.make_async_remote_copy(
            src_ref=to_column.at[pl.ds(1, crossing - 1)], dst_ref=from_column.at[apart],
            send_sem=column_send.at[apart], recv_sem=column_recv.at[apart],
            device_id=(column_peer(apart),), device_id_type=MESH))
    early_copies = []
    for apart in range(1, near):
        early_copies.append(pltpu.make_async_remote_copy(
            src_ref=to_column.at[0], dst_ref=early_ref.at[apart],
            send_sem=early_send.at[apart], recv_sem=early_recv.at[apart],
            device_id=(group_peer(apart),), device_id_type=MESH))
    for copy in column_copies + early_copies:
        copy.start()

    for copy in halo_copies:
        copy.wait_recv()
    for row in range(plan.wide_used, plan.wide_rows):
        wide_f32[pl.ds(row, plan.vectors, stride=PITCH), :] = jnp.zeros((plan.vectors, width), F32)
    wide_f32[pl.ds(base, plan.vectors, stride=PITCH), :] = jnp.dot(beside_ref[0], stencil_ref[0], preferred_element_type=F32)
    wide_f32[pl.ds(base + 1, plan.vectors, stride=PITCH), :] = jnp.dot(beside_ref[1], stencil_ref[2], preferred_element_type=F32)
    for position in range(local):
        lift_wide(position, coarsen(position, every).astype(BF16))
    narrow(starts[2], segments[2])

    sums = [to_column[index].astype(F32) for index in range(crossing)]
    for apart, copy in enumerate(column_copies, 1):
        copy.wait_recv()
        source = lax.rem(place + far - apart, far)
        for index in range(1, crossing):
            reach = plan.groups[plan.crossing[index]] // near
            keep = (source // reach == place // reach).astype(F32)
            sums[index] = sums[index] + keep * from_column[apart, index - 1].astype(F32)
    for index in range(1, crossing):
        to_group[index - 1] = sums[index].astype(BF16)

    back_copies = []
    for apart in range(1, near):
        back_copies.append(pltpu.make_async_remote_copy(
            src_ref=to_group, dst_ref=back.at[apart],
            send_sem=back_send.at[apart], recv_sem=back_recv.at[apart],
            device_id=(group_peer(apart),), device_id_type=MESH))
    for copy in back_copies:
        copy.start()

    result_ref[0, part_of(mine), :] = to_column[0]
    for apart, copy in enumerate(early_copies, 1):
        copy.wait_recv()
        result_ref[0, part_of(lax.rem(mine + near - apart, near)), :] = early_ref[apart]
    lift_wide(local, result_ref[0])

    @pl.when(jnp.logical_not(early))
    def _():
        narrow(starts[1], segments[1])

    narrow(starts[3], segments[3])
    for index in range(1, crossing):
        result_ref[index, part_of(mine), :] = to_group[index - 1]
    for apart, copy in enumerate(back_copies, 1):
        copy.wait_recv()
        source = lax.rem(mine + near - apart, near)
        for index in range(1, crossing):
            result_ref[index, part_of(source), :] = back[apart, index - 1]
    for index in range(1, crossing):
        lift_wide(local + index, result_ref[index])
    for vector in range(plan.vectors):
        table_ref[vector, pl.ds(plan.narrow_rows, plan.wide_rows), :] = (
            wide_f32[pl.ds(vector * PITCH, plan.wide_rows), :].astype(BF16))
    for copy in copies + halo_copies + column_copies + early_copies + back_copies:
        copy.wait_send()


def final_kernel(plan, pieces, spread_ref, table_ref, level0_ref, out_hbm, staged, out_sem):
    width = plan.width
    copies, at = [], 0
    for index, piece in enumerate(pieces):
        for first in range(at, at + piece, 2):
            tables = jnp.concatenate([table_ref[first], table_ref[first + 1]], axis=1)
            both = jnp.dot(spread_ref[...], tables, preferred_element_type=F32)
            staged[first] = both[:, :width] + level0_ref[first]
            staged[first + 1] = both[:, width:] + level0_ref[first + 1]
        here = pl.ds(at, piece)
        copy = pltpu.make_async_copy(staged.at[here], out_hbm.at[here], out_sem.at[index])
        copy.start()
        copies.append(copy)
        at += piece
    for copy in copies:
        copy.wait()


def shards(fine, pattern, stencil, restrict, coarse_inv):
    devices = lax.axis_size("gx")
    vectors, blocks, width = fine.shape
    levels, kinds = restrict.shape[:2]
    plan = Plan(devices, vectors, blocks, width, levels, kinds)
    stacked = restrict.reshape(levels, kinds * width, width)
    eighth = vectors // 8
    segments = (3 * eighth // 2, 2 * eighth, 3 * eighth, 3 * eighth // 2)
    near = plan.groups[plan.crossing[0]]
    far = devices // near
    crossing = len(plan.crossing)
    part = vectors // near
    table_rows = plan.narrow_rows + plan.wide_rows
    vmem = pl.BlockSpec(memory_space=pltpu.VMEM)
    hbm = pl.BlockSpec(memory_space=pltpu.HBM)
    dma = pltpu.SemaphoreType.DMA
    pinned = [pltpu.with_memory_space_constraint(x, pltpu.HBM) for x in (pattern, fine, stacked, coarse_inv, stencil)]
    table, level0, spread = pl.pallas_call(
        functools.partial(exchange_kernel, plan, segments),
        out_shape=(
            pltpu.VMEM((vectors, table_rows, width), BF16),
            pltpu.VMEM((vectors, blocks, width), F32),
            pltpu.VMEM((blocks, table_rows), BF16),
        ),
        in_specs=[hbm] * 5,
        out_specs=(vmem, vmem, vmem),
        scratch_shapes=[
            pltpu.VMEM(pattern.shape, jnp.int32),
            pltpu.VMEM(fine.shape, BF16),
            pltpu.VMEM(stacked.shape, BF16),
            pltpu.VMEM(coarse_inv.shape, BF16),
            pltpu.VMEM(stencil.shape, BF16),
            pltpu.VMEM((vectors * PITCH, width), F32),
            pltpu.VMEM((plan.wide_rows, blocks), BF16),
            pltpu.VMEM((plan.narrow_rows, blocks), BF16),
            pltpu.VMEM((2, part * PITCH, width), F32),
            pltpu.VMEM((max(segments), plan.cut, width), BF16),
            pltpu.VMEM((max(segments), plan.narrow_rows - plan.cut, width), F32),
            pltpu.VMEM((len(plan.narrow), kinds * width, kinds * width), BF16),
            pltpu.VMEM((2 * width, 4 * width), BF16),
            pltpu.VMEM((4, blocks, width), F32),
            pltpu.VMEM((plan.wide_used, vectors, width), BF16),
            pltpu.VMEM((crossing, vectors, width), BF16),
            pltpu.VMEM((crossing, part, width), F32),
            pltpu.VMEM((crossing, vectors, width), BF16),
            pltpu.VMEM((2, vectors, width), BF16),
            pltpu.VMEM((2, vectors, width), BF16),
            pltpu.VMEM((near, crossing, part, width), BF16),
            pltpu.VMEM((crossing, part, width), BF16),
            pltpu.VMEM((near, part, width), BF16),
            pltpu.VMEM((far, crossing - 1, part, width), BF16),
            pltpu.VMEM((crossing - 1, part, width), BF16),
            pltpu.VMEM((near, crossing - 1, part, width), BF16),
            dma((near,)), dma((5,)),
            dma((near,)), dma((near,)), dma((near,)), dma((near,)), dma((far,)), dma((far,)), dma((near,)), dma((near,)), dma((2,)), dma((2,)),
        ],
        compiler_params=pltpu.CompilerParams(
            collective_id=0, has_side_effects=True, vmem_limit_bytes=VMEM_LIMIT),
        name="exchange",
    )(*pinned)

    pieces = [2, 2, 4] + [8] * (vectors // 8 - 2) + [4, 2, 2]
    return pl.pallas_call(
        functools.partial(final_kernel, plan, pieces),
        out_shape=jax.ShapeDtypeStruct(fine.shape, F32),
        in_specs=[vmem, vmem, vmem],
        out_specs=pl.BlockSpec(memory_space=pl.ANY),
        scratch_shapes=[pltpu.VMEM(fine.shape, F32), dma((len(pieces),))],
        compiler_params=pltpu.CompilerParams(vmem_limit_bytes=VMEM_LIMIT),
        name="final",
    )(spread, table, level0)


def solution(mesh):
    in_specs = (P(None, "gx", None), P(None, "gx"), P(), P(), P())
    out_specs = P(None, "gx", None)
    return jax.shard_map(shards, mesh=mesh, in_specs=in_specs, out_specs=out_specs, check_vma=False)
```

```python
import functools

import jax
import jax.numpy as jnp
from jax import lax
from jax.experimental import pallas as pl
from jax.experimental.pallas import tpu as pltpu
from jax.sharding import PartitionSpec as P

MESH = pl.DeviceIdType.MESH
F32 = jnp.float32
BF16 = jnp.bfloat16
TILE = 16
VMEM_LIMIT = 30 * 2**20


def round_up(value, unit):
    return -(-value // unit) * unit


class Plan:
    def __init__(self, devices, vectors, blocks, width, levels, kinds):
        self.devices, self.vectors, self.blocks = devices, vectors, blocks
        self.width, self.levels, self.kinds = width, levels, kinds
        all_blocks = devices * blocks
        self.spans, self.local_spans, self.counts, self.groups = [], [], [], []
        for level in range(levels):
            span = all_blocks // max(all_blocks // 4 ** (level + 1), 1)
            local = min(span, blocks)
            self.spans.append(span)
            self.local_spans.append(local)
            self.counts.append(blocks // local)
            self.groups.append(span // local)
        self.narrow = [l for l in range(levels) if self.counts[l] > 1]
        self.wide = [l for l in range(levels) if self.counts[l] == 1]
        self.crossing = [l for l in range(levels) if self.groups[l] > 1]
        self.padded = {l: round_up(self.counts[l], TILE // 2) for l in self.narrow}
        self.offsets, at = {}, 0
        for l in self.narrow:
            self.offsets[l] = at
            at += kinds * self.padded[l]
        self.narrow_rows = at
        self.small = [l for l in self.narrow if self.padded[l] % TILE]
        self.cut = min([self.offsets[l] for l in self.small], default=at)
        self.narrow_rows = round_up(at, 2 * TILE)
        early = len(self.wide) - len(self.crossing) + 1
        self.base = early * kinds
        self.late_first = round_up(self.base + 2, TILE)
        late = self.late_first - self.base
        self.wide_at = [p * kinds + (late if p >= early else 0) for p in range(len(self.wide))]
        self.wide_end = self.wide_at[-1] + kinds
        self.wide_rows = round_up(self.wide_end, 2 * TILE)
        used = [at + kind for at in self.wide_at for kind in range(kinds)] + [self.base, self.base + 1]
        self.wide_used = sorted(used)


def wide_rows_onehot(plan, pattern, rows_axis):
    shape = (plan.wide_rows, plan.blocks) if rows_axis == 0 else (plan.blocks, plan.wide_rows)
    row = lax.broadcasted_iota(jnp.int32, shape, rows_axis)
    block = lax.broadcasted_iota(jnp.int32, shape, 1 - rows_axis)
    base = plan.base
    hit = ((row == base) & (block == 0)) | ((row == base + 1) & (block == plan.blocks - 1))
    for position, level in enumerate(plan.wide):
        kinds = pattern[level : level + 1, :] if rows_axis == 0 else pattern[:, level : level + 1]
        first = plan.wide_at[position]
        inside = (row >= first) & (row < first + plan.kinds)
        hit = hit | (inside & (row - first == kinds))
    return hit.astype(F32).astype(BF16)


def narrow_onehot(plan, pattern, level, rows_axis):
    padded = plan.padded[level]
    rows = plan.kinds * padded
    shape = (rows, plan.blocks) if rows_axis == 0 else (plan.blocks, rows)
    row = lax.broadcasted_iota(jnp.int32, shape, rows_axis)
    block = lax.broadcasted_iota(jnp.int32, shape, 1 - rows_axis)
    kinds = pattern[level : level + 1, :] if rows_axis == 0 else pattern[:, level : level + 1]
    target = kinds * padded + block // plan.local_spans[level]
    return (row == target).astype(F32).astype(BF16)

PITCH = 40


def exchange_kernel(plan, segments, pattern_hbm, fine_hbm, restrict_hbm, inverse_hbm, stencil_hbm,
                    table_ref, level0_ref, spread_ref,
                    pattern_ref, fine_ref, restrict_ref, inverse_ref, stencil_ref, wide_f32, wide_onehot, onehot, few,
                    grouped, grouped_small, joint, joint_wide, pair_weights, split, rows, coarse_ref, own_ref, result_ref, halo_ref, beside_ref,
                    from_group, to_column, early_ref, from_column, to_group, back,
                    fine_sem, weight_sem, group_send, group_recv,
                    early_send, early_recv, column_send, column_recv, back_send, back_recv, halo_send, halo_recv):
    width, kinds, blocks = plan.width, plan.kinds, plan.blocks
    devices = plan.devices
    near = plan.groups[plan.crossing[0]]
    far = devices // near
    local = len(plan.wide) - len(plan.crossing)
    crossing = len(plan.crossing)
    part = plan.vectors // near
    me = lax.axis_index("gx")
    early = me < 2
    mine = lax.rem(me, near)
    place = me // near

    def part_of(index):
        return pl.ds(pl.multiple_of(index * part, part), part)

    def part_at(turn):
        return lax.rem(mine + 1 + turn, near)

    def fine_copy(turn):
        here = part_of(part_at(turn))
        return pltpu.make_async_copy(fine_hbm.at[here], fine_ref.at[here], fine_sem.at[turn])

    wide_first = plan.wide[0]
    wide_weights = pl.ds(wide_first, len(plan.wide))
    weight_copies = [
        pltpu.make_async_copy(restrict_hbm.at[wide_weights], restrict_ref.at[wide_weights], weight_sem.at[0]),
        pltpu.make_async_copy(restrict_hbm.at[pl.ds(0, wide_first)], restrict_ref.at[pl.ds(0, wide_first)], weight_sem.at[1]),
        pltpu.make_async_copy(inverse_hbm, inverse_ref, weight_sem.at[2]),
        pltpu.make_async_copy(stencil_hbm, stencil_ref, weight_sem.at[3]),
    ]
    pattern_copy = pltpu.make_async_copy(pattern_hbm, pattern_ref, weight_sem.at[4])
    pattern_copy.start()
    for turn in range(near - 1):
        fine_copy(turn).start()
    weight_copies[0].start()
    fine_copy(near - 1).start()
    for copy in weight_copies[1:]:
        copy.start()

    def group_peer(apart):
        return place * near + lax.rem(mine + apart, near)

    def column_peer(apart):
        return lax.rem(place + apart, far) * near + mine

    nexts = lax.rem(me + 1, devices)
    previous = lax.rem(me + devices - 1, devices)
    barrier = pltpu.get_barrier_semaphore()
    peers = [group_peer(a) for a in range(1, near)] + [column_peer(a) for a in range(1, far)] + [nexts, previous]
    for peer in peers:
        pl.semaphore_signal(barrier, inc=1, device_id=(peer,), device_id_type=MESH)

    pattern_copy.wait()
    wide_onehot[...] = wide_rows_onehot(plan, pattern_ref[...], 0)
    for level in plan.narrow:
        onehot[pl.ds(plan.offsets[level], kinds * plan.padded[level]), :] = narrow_onehot(
            plan, pattern_ref[...], level, 0)
    turned = pattern_ref[...].T
    for level in plan.narrow:
        columns = pl.ds(plan.offsets[level], kinds * plan.padded[level])
        spread_ref[:, columns] = narrow_onehot(plan, turned, level, 1)
    spread_ref[:, pl.ds(plan.narrow_rows, plan.wide_rows)] = wide_rows_onehot(plan, turned, 1)

    for row in plan.wide_used:
        rows[row, part_of(mine), :] = jnp.zeros((part, width), BF16)

    def gather(turn):
        fine_copy(turn).wait()
        for first in range(0, part, 2):
            at = part_at(turn) * part + first
            both = jnp.concatenate([fine_ref[at], fine_ref[at + 1]], axis=1)
            both = jnp.dot(wide_onehot[...], both, preferred_element_type=F32)
            few[turn % 2, pl.ds(first * PITCH, plan.wide_rows), :] = both[:, :width]
            few[turn % 2, pl.ds((first + 1) * PITCH, plan.wide_rows), :] = both[:, width:]

    def extract(turn):
        for row in plan.wide_used:
            rows[row, part_of(part_at(turn)), :] = few[turn % 2, pl.ds(row, part, stride=PITCH), :].astype(BF16)

    def coarsen(position, vectors):
        level, first = plan.wide[position], plan.wide_at[position]
        joined = jnp.concatenate([rows[first + kind, vectors, :] for kind in range(kinds)], axis=1)
        coarse = jnp.dot(joined, restrict_ref[level], preferred_element_type=F32)
        return coarse * plan.spans[level] ** (-0.5)

    every = pl.ds(0, plan.vectors)
    for turn in range(near - 1):
        gather(turn)
        if turn > 0:
            extract(turn - 1)
    extract(near - 2)
    weight_copies[0].wait()
    for index in range(crossing):
        coarse_ref[index] = coarsen(local + index, every).astype(BF16)

    pl.semaphore_wait(barrier, len(peers))

    copies = []
    for apart in range(1, near):
        theirs = lax.rem(mine + apart, near)
        copies.append(pltpu.make_async_remote_copy(
            src_ref=coarse_ref.at[:, part_of(theirs), :],
            dst_ref=from_group.at[apart],
            send_sem=group_send.at[apart], recv_sem=group_recv.at[apart],
            device_id=(group_peer(apart),), device_id_type=MESH))
    for copy in copies:
        copy.start()

    gather(near - 1)
    extract(near - 1)
    for index in range(crossing):
        own_ref[index] = coarsen(local + index, part_of(mine))
    base = plan.base
    halo_ref[0] = rows[base]
    halo_ref[1] = rows[base + 1]
    halo_copies = []
    for side, peer in ((0, previous), (1, nexts)):
        halo_copies.append(pltpu.make_async_remote_copy(
            src_ref=halo_ref.at[side], dst_ref=beside_ref.at[1 - side],
            send_sem=halo_send.at[side], recv_sem=halo_recv.at[1 - side],
            device_id=(peer,), device_id_type=MESH))
    for copy in halo_copies:
        copy.start()

    for copy in weight_copies[1:]:
        copy.wait()
    for position, level in enumerate(plan.narrow):
        half = jnp.dot(restrict_ref[level], inverse_ref[level], preferred_element_type=F32).astype(BF16)
        full = lax.dot_general(half, restrict_ref[level], (((1,), (1,)), ((), ())), preferred_element_type=F32)
        joint[position] = (full * plan.spans[level] ** (-0.5)).astype(BF16)

    none = jnp.zeros((width, width), BF16)
    pair_weights[...] = jnp.concatenate([
        jnp.concatenate([stencil_ref[1], stencil_ref[0], none, stencil_ref[2]], axis=1),
        jnp.concatenate([stencil_ref[2], stencil_ref[1], stencil_ref[0], none], axis=1)], axis=0)
    pairs = blocks // 2
    edge = lax.broadcasted_iota(jnp.int32, (pairs, width), 0)
    ahead = (edge > 0).astype(F32)
    behind = (edge < pairs - 1).astype(F32)

    def narrow(start, chunk):
        for slot in range(0, chunk, 2):
            at = start + slot
            both = jnp.concatenate([fine_ref[at], fine_ref[at + 1]], axis=1)
            both = jnp.dot(onehot[...], both, preferred_element_type=F32)
            large = both[: plan.cut].astype(BF16)
            grouped[slot] = large[:, :width]
            grouped[slot + 1] = large[:, width:]
            grouped_small[slot] = both[plan.cut :, :width]
            grouped_small[slot + 1] = both[plan.cut :, width:]
        for slot in range(chunk):
            at = start + slot
            turn = slot % 4
            split[turn] = fine_ref[at].astype(F32)
            evens = split[turn, pl.ds(0, pairs, stride=2), :].astype(BF16)
            odds = split[turn, pl.ds(1, pairs, stride=2), :].astype(BF16)
            four = jnp.dot(jnp.concatenate([evens, odds], axis=1), pair_weights[...], preferred_element_type=F32)
            earlier = pltpu.roll(four[:, 2 * width : 3 * width], 1, 0) * ahead
            later = pltpu.roll(four[:, 3 * width :], pairs - 1, 0) * behind
            level0_ref[at, pl.ds(0, pairs, stride=2), :] = four[:, :width] + earlier
            level0_ref[at, pl.ds(1, pairs, stride=2), :] = four[:, width : 2 * width] + later
        for position, level in enumerate(plan.narrow):
            padded = plan.padded[level]
            small = level in plan.small
            source, first = (grouped_small, plan.cut) if small else (grouped, 0)
            slices = [pl.ds(plan.offsets[level] - first + kind * padded, padded) for kind in range(kinds)]
            joined = jnp.concatenate(
                [source[pl.ds(0, chunk), tile, :].reshape(chunk * padded, width).astype(BF16) for tile in slices], axis=1)
            lifted = jnp.dot(joined, joint[position], preferred_element_type=F32)
            tiles = [lifted[:, kind * width : (kind + 1) * width].reshape(chunk, padded, width) for kind in range(kinds)]
            target = pl.ds(plan.offsets[level], kinds * padded)
            table_ref[pl.ds(start, chunk), target, :] = jnp.concatenate(tiles, axis=1).astype(BF16)

    def lift_wide(position, rounded):
        level = plan.wide[position]
        if position > local:
            lifted = jnp.dot(rounded, joint_wide[position - local - 1], preferred_element_type=F32)
        else:
            solved = jnp.dot(rounded, inverse_ref[level], preferred_element_type=F32).astype(BF16)
            lifted = lax.dot_general(
                solved, restrict_ref[level], (((1,), (1,)), ((), ())), preferred_element_type=F32)
        for kind in range(kinds):
            wide_f32[pl.ds(plan.wide_at[position] + kind, plan.vectors, stride=PITCH), :] = (
                lifted[:, kind * width : (kind + 1) * width])

    starts = [sum(segments[:index]) for index in range(len(segments))]
    narrow(starts[0], segments[0])

    @pl.when(early)
    def _():
        narrow(starts[1], segments[1])


    total = own_ref[...]
    for apart, copy in enumerate(copies, 1):
        copy.wait_recv()
        total = total + from_group[apart].astype(F32)
    to_column[...] = total.astype(BF16)

    column_copies = []
    for apart in range(1, far):
        column_copies.append(pltpu.make_async_remote_copy(
            src_ref=to_column.at[pl.ds(1, crossing - 1)], dst_ref=from_column.at[apart],
            send_sem=column_send.at[apart], recv_sem=column_recv.at[apart],
            device_id=(column_peer(apart),), device_id_type=MESH))
    early_copies = []
    for apart in range(1, near):
        early_copies.append(pltpu.make_async_remote_copy(
            src_ref=to_column.at[0], dst_ref=early_ref.at[apart],
            send_sem=early_send.at[apart], recv_sem=early_recv.at[apart],
            device_id=(group_peer(apart),), device_id_type=MESH))
    for copy in column_copies + early_copies:
        copy.start()

    for copy in halo_copies:
        copy.wait_recv()
    for row in sorted(set(range(plan.wide_rows)) - set(plan.wide_used)):
        wide_f32[pl.ds(row, plan.vectors, stride=PITCH), :] = jnp.zeros((plan.vectors, width), F32)
    wide_f32[pl.ds(base, plan.vectors, stride=PITCH), :] = jnp.dot(beside_ref[0], stencil_ref[0], preferred_element_type=F32)
    wide_f32[pl.ds(base + 1, plan.vectors, stride=PITCH), :] = jnp.dot(beside_ref[1], stencil_ref[2], preferred_element_type=F32)
    for index in range(1, crossing):
        level = plan.crossing[index]
        joint_wide[index - 1] = lax.dot_general(
            inverse_ref[level], restrict_ref[level], (((1,), (1,)), ((), ())),
            preferred_element_type=F32).astype(BF16)
    for position in range(local):
        lift_wide(position, coarsen(position, every).astype(BF16))
    narrow(starts[2], segments[2])

    sums = [to_column[index].astype(F32) for index in range(crossing)]
    for apart, copy in enumerate(column_copies, 1):
        copy.wait_recv()
        source = lax.rem(place + far - apart, far)
        for index in range(1, crossing):
            reach = plan.groups[plan.crossing[index]] // near
            keep = (source // reach == place // reach).astype(F32)
            sums[index] = sums[index] + keep * from_column[apart, index - 1].astype(F32)
    for index in range(1, crossing):
        to_group[index - 1] = sums[index].astype(BF16)

    back_copies = []
    for apart in range(1, near):
        back_copies.append(pltpu.make_async_remote_copy(
            src_ref=to_group, dst_ref=back.at[apart],
            send_sem=back_send.at[apart], recv_sem=back_recv.at[apart],
            device_id=(group_peer(apart),), device_id_type=MESH))
    for copy in back_copies:
        copy.start()

    result_ref[0, part_of(mine), :] = to_column[0]
    for apart, copy in enumerate(early_copies, 1):
        copy.wait_recv()
        result_ref[0, part_of(lax.rem(mine + near - apart, near)), :] = early_ref[apart]
    lift_wide(local, result_ref[0])

    def fill(first, stop):
        for vector in range(plan.vectors):
            table_ref[vector, pl.ds(plan.narrow_rows + first, stop - first), :] = (
                wide_f32[pl.ds(vector * PITCH + first, stop - first), :].astype(BF16))

    fill(0, plan.late_first)

    @pl.when(jnp.logical_not(early))
    def _():
        narrow(starts[1], segments[1])

    narrow(starts[3], segments[3])
    for index in range(1, crossing):
        result_ref[index, part_of(mine), :] = to_group[index - 1]
    for apart, copy in enumerate(back_copies, 1):
        copy.wait_recv()
        source = lax.rem(mine + near - apart, near)
        for index in range(1, crossing):
            result_ref[index, part_of(source), :] = back[apart, index - 1]
    for index in range(1, crossing):
        lift_wide(local + index, result_ref[index])
    fill(plan.late_first, plan.wide_rows)
    for copy in copies + halo_copies + column_copies + early_copies + back_copies:
        copy.wait_send()


def final_kernel(plan, pieces, spread_ref, table_ref, level0_ref, out_hbm, staged, out_sem):
    width = plan.width
    copies, at = [], 0
    for index, piece in enumerate(pieces):
        for first in range(at, at + piece, 2):
            tables = jnp.concatenate([table_ref[first], table_ref[first + 1]], axis=1)
            both = jnp.dot(spread_ref[...], tables, preferred_element_type=F32)
            staged[first] = both[:, :width] + level0_ref[first]
            staged[first + 1] = both[:, width:] + level0_ref[first + 1]
        here = pl.ds(at, piece)
        copy = pltpu.make_async_copy(staged.at[here], out_hbm.at[here], out_sem.at[index])
        copy.start()
        copies.append(copy)
        at += piece
    for copy in copies:
        copy.wait()


def shards(fine, pattern, stencil, restrict, coarse_inv):
    devices = lax.axis_size("gx")
    vectors, blocks, width = fine.shape
    levels, kinds = restrict.shape[:2]
    plan = Plan(devices, vectors, blocks, width, levels, kinds)
    stacked = restrict.reshape(levels, kinds * width, width)
    eighth = vectors // 8
    segments = (3 * eighth // 2, 2 * eighth, 3 * eighth, 3 * eighth // 2)
    near = plan.groups[plan.crossing[0]]
    far = devices // near
    crossing = len(plan.crossing)
    part = vectors // near
    table_rows = plan.narrow_rows + plan.wide_rows
    vmem = pl.BlockSpec(memory_space=pltpu.VMEM)
    hbm = pl.BlockSpec(memory_space=pltpu.HBM)
    dma = pltpu.SemaphoreType.DMA
    pinned = [pltpu.with_memory_space_constraint(x, pltpu.HBM) for x in (pattern, fine, stacked, coarse_inv, stencil)]
    table, level0, spread = pl.pallas_call(
        functools.partial(exchange_kernel, plan, segments),
        out_shape=(
            pltpu.VMEM((vectors, table_rows, width), BF16),
            pltpu.VMEM((vectors, blocks, width), F32),
            pltpu.VMEM((blocks, table_rows), BF16),
        ),
        in_specs=[hbm] * 5,
        out_specs=(vmem, vmem, vmem),
        scratch_shapes=[
            pltpu.VMEM(pattern.shape, jnp.int32),
            pltpu.VMEM(fine.shape, BF16),
            pltpu.VMEM(stacked.shape, BF16),
            pltpu.VMEM(coarse_inv.shape, BF16),
            pltpu.VMEM(stencil.shape, BF16),
            pltpu.VMEM((vectors * PITCH, width), F32),
            pltpu.VMEM((plan.wide_rows, blocks), BF16),
            pltpu.VMEM((plan.narrow_rows, blocks), BF16),
            pltpu.VMEM((2, part * PITCH, width), F32),
            pltpu.VMEM((max(segments), plan.cut, width), BF16),
            pltpu.VMEM((max(segments), plan.narrow_rows - plan.cut, width), F32),
            pltpu.VMEM((len(plan.narrow), kinds * width, kinds * width), BF16),
            pltpu.VMEM((crossing - 1, width, kinds * width), BF16),
            pltpu.VMEM((2 * width, 4 * width), BF16),
            pltpu.VMEM((4, blocks, width), F32),
            pltpu.VMEM((plan.wide_end, vectors, width), BF16),
            pltpu.VMEM((crossing, vectors, width), BF16),
            pltpu.VMEM((crossing, part, width), F32),
            pltpu.VMEM((crossing, vectors, width), BF16),
            pltpu.VMEM((2, vectors, width), BF16),
            pltpu.VMEM((2, vectors, width), BF16),
            pltpu.VMEM((near, crossing, part, width), BF16),
            pltpu.VMEM((crossing, part, width), BF16),
            pltpu.VMEM((near, part, width), BF16),
            pltpu.VMEM((far, crossing - 1, part, width), BF16),
            pltpu.VMEM((crossing - 1, part, width), BF16),
            pltpu.VMEM((near, crossing - 1, part, width), BF16),
            dma((near,)), dma((5,)),
            dma((near,)), dma((near,)), dma((near,)), dma((near,)), dma((far,)), dma((far,)), dma((near,)), dma((near,)), dma((2,)), dma((2,)),
        ],
        compiler_params=pltpu.CompilerParams(
            collective_id=0, has_side_effects=True, vmem_limit_bytes=VMEM_LIMIT),
        name="exchange",
    )(*pinned)

    pieces = [4] * (vectors // 4)
    return pl.pallas_call(
        functools.partial(final_kernel, plan, pieces),
        out_shape=jax.ShapeDtypeStruct(fine.shape, F32),
        in_specs=[vmem, vmem, vmem],
        out_specs=pl.BlockSpec(memory_space=pl.ANY),
        scratch_shapes=[pltpu.VMEM(fine.shape, F32), dma((len(pieces),))],
        compiler_params=pltpu.CompilerParams(vmem_limit_bytes=VMEM_LIMIT),
        name="final",
    )(spread, table, level0)


def solution(mesh):
    in_specs = (P(None, "gx", None), P(None, "gx"), P(), P(), P())
    out_specs = P(None, "gx", None)
    return jax.shard_map(shards, mesh=mesh, in_specs=in_specs, out_specs=out_specs, check_vma=False)
```

```python
import functools

import jax
import jax.numpy as jnp
from jax import lax
from jax.experimental import pallas as pl
from jax.experimental.pallas import tpu as pltpu
from jax.sharding import PartitionSpec as P

MESH = pl.DeviceIdType.MESH
F32 = jnp.float32
BF16 = jnp.bfloat16
TILE = 16
VMEM_LIMIT = 30 * 2**20


def round_up(value, unit):
    return -(-value // unit) * unit


class Plan:
    def __init__(self, devices, vectors, blocks, width, levels, kinds):
        self.devices, self.vectors, self.blocks = devices, vectors, blocks
        self.width, self.levels, self.kinds = width, levels, kinds
        all_blocks = devices * blocks
        self.spans, self.local_spans, self.counts, self.groups = [], [], [], []
        for level in range(levels):
            span = all_blocks // max(all_blocks // 4 ** (level + 1), 1)
            local = min(span, blocks)
            self.spans.append(span)
            self.local_spans.append(local)
            self.counts.append(blocks // local)
            self.groups.append(span // local)
        self.narrow = [l for l in range(levels) if self.counts[l] > 1]
        self.wide = [l for l in range(levels) if self.counts[l] == 1]
        self.crossing = [l for l in range(levels) if self.groups[l] > 1]
        self.padded = {l: round_up(self.counts[l], TILE // 2) for l in self.narrow}
        self.offsets, at = {}, 0
        for l in self.narrow:
            self.offsets[l] = at
            at += kinds * self.padded[l]
        self.narrow_rows = at
        self.small = [l for l in self.narrow if self.padded[l] % TILE]
        self.cut = min([self.offsets[l] for l in self.small], default=at)
        self.narrow_rows = round_up(at, 2 * TILE)
        early = len(self.wide) - len(self.crossing) + 1
        self.base = early * kinds
        self.late_first = round_up(self.base + 2, TILE)
        late = self.late_first - self.base
        self.wide_at = [p * kinds + (late if p >= early else 0) for p in range(len(self.wide))]
        self.wide_end = self.wide_at[-1] + kinds
        self.wide_rows = round_up(self.wide_end, 2 * TILE)
        used = [at + kind for at in self.wide_at for kind in range(kinds)] + [self.base, self.base + 1]
        self.wide_used = sorted(used)


def wide_rows_onehot(plan, pattern, rows_axis):
    shape = (plan.wide_rows, plan.blocks) if rows_axis == 0 else (plan.blocks, plan.wide_rows)
    row = lax.broadcasted_iota(jnp.int32, shape, rows_axis)
    block = lax.broadcasted_iota(jnp.int32, shape, 1 - rows_axis)
    base = plan.base
    hit = ((row == base) & (block == 0)) | ((row == base + 1) & (block == plan.blocks - 1))
    for position, level in enumerate(plan.wide):
        kinds = pattern[level : level + 1, :] if rows_axis == 0 else pattern[:, level : level + 1]
        first = plan.wide_at[position]
        inside = (row >= first) & (row < first + plan.kinds)
        hit = hit | (inside & (row - first == kinds))
    return hit.astype(F32).astype(BF16)


def narrow_onehot(plan, pattern, level, rows_axis):
    padded = plan.padded[level]
    rows = plan.kinds * padded
    shape = (rows, plan.blocks) if rows_axis == 0 else (plan.blocks, rows)
    row = lax.broadcasted_iota(jnp.int32, shape, rows_axis)
    block = lax.broadcasted_iota(jnp.int32, shape, 1 - rows_axis)
    kinds = pattern[level : level + 1, :] if rows_axis == 0 else pattern[:, level : level + 1]
    target = kinds * padded + block // plan.local_spans[level]
    return (row == target).astype(F32).astype(BF16)

PITCH = 40


def exchange_kernel(plan, segments, pattern_hbm, fine_hbm, restrict_hbm, inverse_hbm, stencil_hbm,
                    table_ref, level0_ref, spread_ref,
                    pattern_ref, fine_ref, restrict_ref, inverse_ref, stencil_ref, wide_f32, wide_onehot, onehot, few,
                    grouped, grouped_small, joint, joint_wide, pair_weights, split, rows, coarse_ref, own_ref, result_ref, halo_ref, beside_ref,
                    from_group, to_column, early_ref, from_column, to_group, back,
                    fine_sem, weight_sem, group_send, group_recv,
                    early_send, early_recv, column_send, column_recv, back_send, back_recv, halo_send, halo_recv):
    width, kinds, blocks = plan.width, plan.kinds, plan.blocks
    devices = plan.devices
    near = plan.groups[plan.crossing[0]]
    far = devices // near
    local = len(plan.wide) - len(plan.crossing)
    crossing = len(plan.crossing)
    part = plan.vectors // near
    me = lax.axis_index("gx")
    early = me < 2
    mine = lax.rem(me, near)
    place = me // near

    def part_of(index):
        return pl.ds(pl.multiple_of(index * part, part), part)

    def part_at(turn):
        return lax.rem(mine + 1 + turn, near)

    def fine_copy(turn):
        here = part_of(part_at(turn))
        return pltpu.make_async_copy(fine_hbm.at[here], fine_ref.at[here], fine_sem.at[turn])

    wide_first = plan.wide[0]
    wide_weights = pl.ds(wide_first, len(plan.wide))
    weight_copies = [
        pltpu.make_async_copy(restrict_hbm.at[wide_weights], restrict_ref.at[wide_weights], weight_sem.at[0]),
        pltpu.make_async_copy(restrict_hbm.at[pl.ds(0, wide_first)], restrict_ref.at[pl.ds(0, wide_first)], weight_sem.at[1]),
        pltpu.make_async_copy(inverse_hbm, inverse_ref, weight_sem.at[2]),
        pltpu.make_async_copy(stencil_hbm, stencil_ref, weight_sem.at[3]),
    ]
    pattern_copy = pltpu.make_async_copy(pattern_hbm, pattern_ref, weight_sem.at[4])
    pattern_copy.start()
    for turn in range(near - 1):
        fine_copy(turn).start()
    weight_copies[0].start()
    fine_copy(near - 1).start()
    for copy in weight_copies[1:]:
        copy.start()

    def group_peer(apart):
        return place * near + lax.rem(mine + apart, near)

    def column_peer(apart):
        return lax.rem(place + apart, far) * near + mine

    nexts = lax.rem(me + 1, devices)
    previous = lax.rem(me + devices - 1, devices)
    barrier = pltpu.get_barrier_semaphore()
    peers = [group_peer(a) for a in range(1, near)] + [column_peer(a) for a in range(1, far)] + [nexts, previous]
    for peer in peers:
        pl.semaphore_signal(barrier, inc=1, device_id=(peer,), device_id_type=MESH)

    pattern_copy.wait()
    wide_onehot[...] = wide_rows_onehot(plan, pattern_ref[...], 0)
    for level in plan.narrow:
        onehot[pl.ds(plan.offsets[level], kinds * plan.padded[level]), :] = narrow_onehot(
            plan, pattern_ref[...], level, 0)
    turned = pattern_ref[...].T
    for level in plan.narrow:
        columns = pl.ds(plan.offsets[level], kinds * plan.padded[level])
        spread_ref[:, columns] = narrow_onehot(plan, turned, level, 1)
    spread_ref[:, pl.ds(plan.narrow_rows, plan.wide_rows)] = wide_rows_onehot(plan, turned, 1)

    for row in plan.wide_used:
        rows[row, part_of(mine), :] = jnp.zeros((part, width), BF16)

    def gather(turn):
        fine_copy(turn).wait()
        for first in range(0, part, 2):
            at = part_at(turn) * part + first
            both = jnp.concatenate([fine_ref[at], fine_ref[at + 1]], axis=1)
            both = jnp.dot(wide_onehot[...], both, preferred_element_type=F32)
            few[turn % 2, pl.ds(first * PITCH, plan.wide_rows), :] = both[:, :width]
            few[turn % 2, pl.ds((first + 1) * PITCH, plan.wide_rows), :] = both[:, width:]

    def extract(turn):
        for row in plan.wide_used:
            rows[row, part_of(part_at(turn)), :] = few[turn % 2, pl.ds(row, part, stride=PITCH), :].astype(BF16)

    def coarsen(position, vectors):
        level, first = plan.wide[position], plan.wide_at[position]
        joined = jnp.concatenate([rows[first + kind, vectors, :] for kind in range(kinds)], axis=1)
        coarse = jnp.dot(joined, restrict_ref[level], preferred_element_type=F32)
        return coarse * plan.spans[level] ** (-0.5)

    every = pl.ds(0, plan.vectors)
    for turn in range(near - 1):
        gather(turn)
        if turn > 0:
            extract(turn - 1)
    extract(near - 2)
    weight_copies[0].wait()
    for index in range(crossing):
        coarse_ref[index] = coarsen(local + index, every).astype(BF16)

    pl.semaphore_wait(barrier, len(peers))

    copies = []
    for apart in range(1, near):
        theirs = lax.rem(mine + apart, near)
        copies.append(pltpu.make_async_remote_copy(
            src_ref=coarse_ref.at[:, part_of(theirs), :],
            dst_ref=from_group.at[apart],
            send_sem=group_send.at[apart], recv_sem=group_recv.at[apart],
            device_id=(group_peer(apart),), device_id_type=MESH))
    for copy in copies:
        copy.start()

    gather(near - 1)
    extract(near - 1)
    for index in range(crossing):
        own_ref[index] = coarsen(local + index, part_of(mine))
    base = plan.base
    halo_ref[0] = rows[base]
    halo_ref[1] = rows[base + 1]
    halo_copies = []
    for side, peer in ((0, previous), (1, nexts)):
        halo_copies.append(pltpu.make_async_remote_copy(
            src_ref=halo_ref.at[side], dst_ref=beside_ref.at[1 - side],
            send_sem=halo_send.at[side], recv_sem=halo_recv.at[1 - side],
            device_id=(peer,), device_id_type=MESH))
    for copy in halo_copies:
        copy.start()

    for copy in weight_copies[1:]:
        copy.wait()
    for position, level in enumerate(plan.narrow):
        half = jnp.dot(restrict_ref[level], inverse_ref[level], preferred_element_type=F32).astype(BF16)
        full = lax.dot_general(half, restrict_ref[level], (((1,), (1,)), ((), ())), preferred_element_type=F32)
        joint[position] = (full * plan.spans[level] ** (-0.5)).astype(BF16)

    none = jnp.zeros((width, width), BF16)
    pair_weights[...] = jnp.concatenate([
        jnp.concatenate([stencil_ref[1], stencil_ref[0], none, stencil_ref[2]], axis=1),
        jnp.concatenate([stencil_ref[2], stencil_ref[1], stencil_ref[0], none], axis=1)], axis=0)
    pairs = blocks // 2
    edge = lax.broadcasted_iota(jnp.int32, (pairs, width), 0)
    ahead = (edge > 0).astype(F32)
    behind = (edge < pairs - 1).astype(F32)

    def narrow(start, chunk):
        for slot in range(0, chunk, 2):
            at = start + slot
            both = jnp.concatenate([fine_ref[at], fine_ref[at + 1]], axis=1)
            both = jnp.dot(onehot[...], both, preferred_element_type=F32)
            large = both[: plan.cut].astype(BF16)
            grouped[slot] = large[:, :width]
            grouped[slot + 1] = large[:, width:]
            grouped_small[slot] = both[plan.cut :, :width]
            grouped_small[slot + 1] = both[plan.cut :, width:]
        for slot in range(chunk):
            at = start + slot
            turn = slot % 4
            split[turn] = fine_ref[at].astype(F32)
            evens = split[turn, pl.ds(0, pairs, stride=2), :].astype(BF16)
            odds = split[turn, pl.ds(1, pairs, stride=2), :].astype(BF16)
            four = jnp.dot(jnp.concatenate([evens, odds], axis=1), pair_weights[...], preferred_element_type=F32)
            earlier = pltpu.roll(four[:, 2 * width : 3 * width], 1, 0) * ahead
            later = pltpu.roll(four[:, 3 * width :], pairs - 1, 0) * behind
            level0_ref[at, pl.ds(0, pairs, stride=2), :] = four[:, :width] + earlier
            level0_ref[at, pl.ds(1, pairs, stride=2), :] = four[:, width : 2 * width] + later
        for position, level in enumerate(plan.narrow):
            padded = plan.padded[level]
            small = level in plan.small
            source, first = (grouped_small, plan.cut) if small else (grouped, 0)
            slices = [pl.ds(plan.offsets[level] - first + kind * padded, padded) for kind in range(kinds)]
            joined = jnp.concatenate(
                [source[pl.ds(0, chunk), tile, :].reshape(chunk * padded, width).astype(BF16) for tile in slices], axis=1)
            lifted = jnp.dot(joined, joint[position], preferred_element_type=F32)
            tiles = [lifted[:, kind * width : (kind + 1) * width].reshape(chunk, padded, width) for kind in range(kinds)]
            target = pl.ds(plan.offsets[level], kinds * padded)
            table_ref[pl.ds(start, chunk), target, :] = jnp.concatenate(tiles, axis=1).astype(BF16)

    def lift_wide(position, rounded):
        level = plan.wide[position]
        if position > local:
            lifted = jnp.dot(rounded, joint_wide[position - local - 1], preferred_element_type=F32)
        else:
            solved = jnp.dot(rounded, inverse_ref[level], preferred_element_type=F32).astype(BF16)
            lifted = lax.dot_general(
                solved, restrict_ref[level], (((1,), (1,)), ((), ())), preferred_element_type=F32)
        for kind in range(kinds):
            wide_f32[pl.ds(plan.wide_at[position] + kind, plan.vectors, stride=PITCH), :] = (
                lifted[:, kind * width : (kind + 1) * width])

    starts = [sum(segments[:index]) for index in range(len(segments))]
    narrow(starts[0], segments[0])

    @pl.when(early)
    def _():
        narrow(starts[1], segments[1])


    total = own_ref[...]
    for apart, copy in enumerate(copies, 1):
        copy.wait_recv()
        total = total + from_group[apart].astype(F32)
    to_column[...] = total.astype(BF16)

    column_copies = []
    for apart in range(1, far):
        column_copies.append(pltpu.make_async_remote_copy(
            src_ref=to_column.at[pl.ds(1, crossing - 1)], dst_ref=from_column.at[apart],
            send_sem=column_send.at[apart], recv_sem=column_recv.at[apart],
            device_id=(column_peer(apart),), device_id_type=MESH))
    early_copies = []
    for apart in range(1, near):
        early_copies.append(pltpu.make_async_remote_copy(
            src_ref=to_column.at[0], dst_ref=early_ref.at[apart],
            send_sem=early_send.at[apart], recv_sem=early_recv.at[apart],
            device_id=(group_peer(apart),), device_id_type=MESH))
    for copy in column_copies + early_copies:
        copy.start()

    for copy in halo_copies:
        copy.wait_recv()
    for row in sorted(set(range(plan.wide_rows)) - set(plan.wide_used)):
        wide_f32[pl.ds(row, plan.vectors, stride=PITCH), :] = jnp.zeros((plan.vectors, width), F32)
    wide_f32[pl.ds(base, plan.vectors, stride=PITCH), :] = jnp.dot(beside_ref[0], stencil_ref[0], preferred_element_type=F32)
    wide_f32[pl.ds(base + 1, plan.vectors, stride=PITCH), :] = jnp.dot(beside_ref[1], stencil_ref[2], preferred_element_type=F32)
    for index in range(1, crossing):
        level = plan.crossing[index]
        joint_wide[index - 1] = lax.dot_general(
            inverse_ref[level], restrict_ref[level], (((1,), (1,)), ((), ())),
            preferred_element_type=F32).astype(BF16)
    for position in range(local):
        lift_wide(position, coarsen(position, every).astype(BF16))
    narrow(starts[2], segments[2])

    sums = [to_column[index].astype(F32) for index in range(crossing)]
    for apart, copy in enumerate(column_copies, 1):
        copy.wait_recv()
        source = lax.rem(place + far - apart, far)
        for index in range(1, crossing):
            reach = plan.groups[plan.crossing[index]] // near
            keep = (source // reach == place // reach).astype(F32)
            sums[index] = sums[index] + keep * from_column[apart, index - 1].astype(F32)
    for index in range(1, crossing):
        to_group[index - 1] = sums[index].astype(BF16)

    back_copies = []
    for apart in range(1, near):
        back_copies.append(pltpu.make_async_remote_copy(
            src_ref=to_group, dst_ref=back.at[apart],
            send_sem=back_send.at[apart], recv_sem=back_recv.at[apart],
            device_id=(group_peer(apart),), device_id_type=MESH))
    for copy in back_copies:
        copy.start()

    result_ref[0, part_of(mine), :] = to_column[0]
    for apart, copy in enumerate(early_copies, 1):
        copy.wait_recv()
        result_ref[0, part_of(lax.rem(mine + near - apart, near)), :] = early_ref[apart]
    lift_wide(local, result_ref[0])

    def fill(first, stop):
        for vector in range(plan.vectors):
            table_ref[vector, pl.ds(plan.narrow_rows + first, stop - first), :] = (
                wide_f32[pl.ds(vector * PITCH + first, stop - first), :].astype(BF16))

    fill(0, plan.late_first)

    @pl.when(jnp.logical_not(early))
    def _():
        narrow(starts[1], segments[1])

    narrow(starts[3], segments[3])
    for index in range(1, crossing):
        result_ref[index, part_of(mine), :] = to_group[index - 1]
    for apart, copy in enumerate(back_copies, 1):
        copy.wait_recv()
        source = lax.rem(mine + near - apart, near)
        for index in range(1, crossing):
            result_ref[index, part_of(source), :] = back[apart, index - 1]
    for index in range(1, crossing):
        lift_wide(local + index, result_ref[index])
    fill(plan.late_first, plan.wide_rows)
    for copy in copies + halo_copies + column_copies + early_copies + back_copies:
        copy.wait_send()


def final_kernel(plan, pieces, spread_ref, table_ref, level0_ref, out_hbm, staged, out_sem):
    width = plan.width
    copies, at = [], 0
    for index, piece in enumerate(pieces):
        for first in range(at, at + piece, 2):
            tables = jnp.concatenate([table_ref[first], table_ref[first + 1]], axis=1)
            both = jnp.dot(spread_ref[...], tables, preferred_element_type=F32)
            staged[first] = both[:, :width] + level0_ref[first]
            staged[first + 1] = both[:, width:] + level0_ref[first + 1]
        here = pl.ds(at, piece)
        copy = pltpu.make_async_copy(staged.at[here], out_hbm.at[here], out_sem.at[index])
        copy.start()
        copies.append(copy)
        at += piece
    for copy in copies:
        copy.wait()


def shards(fine, pattern, stencil, restrict, coarse_inv):
    devices = lax.axis_size("gx")
    vectors, blocks, width = fine.shape
    levels, kinds = restrict.shape[:2]
    plan = Plan(devices, vectors, blocks, width, levels, kinds)
    stacked = restrict.reshape(levels, kinds * width, width)
    eighth = vectors // 8
    segments = (eighth, 2 * eighth, 7 * eighth // 2, 3 * eighth // 2)
    near = plan.groups[plan.crossing[0]]
    far = devices // near
    crossing = len(plan.crossing)
    part = vectors // near
    table_rows = plan.narrow_rows + plan.wide_rows
    vmem = pl.BlockSpec(memory_space=pltpu.VMEM)
    hbm = pl.BlockSpec(memory_space=pltpu.HBM)
    dma = pltpu.SemaphoreType.DMA
    pinned = [pltpu.with_memory_space_constraint(x, pltpu.HBM) for x in (pattern, fine, stacked, coarse_inv, stencil)]
    table, level0, spread = pl.pallas_call(
        functools.partial(exchange_kernel, plan, segments),
        out_shape=(
            pltpu.VMEM((vectors, table_rows, width), BF16),
            pltpu.VMEM((vectors, blocks, width), F32),
            pltpu.VMEM((blocks, table_rows), BF16),
        ),
        in_specs=[hbm] * 5,
        out_specs=(vmem, vmem, vmem),
        scratch_shapes=[
            pltpu.VMEM(pattern.shape, jnp.int32),
            pltpu.VMEM(fine.shape, BF16),
            pltpu.VMEM(stacked.shape, BF16),
            pltpu.VMEM(coarse_inv.shape, BF16),
            pltpu.VMEM(stencil.shape, BF16),
            pltpu.VMEM((vectors * PITCH, width), F32),
            pltpu.VMEM((plan.wide_rows, blocks), BF16),
            pltpu.VMEM((plan.narrow_rows, blocks), BF16),
            pltpu.VMEM((2, part * PITCH, width), F32),
            pltpu.VMEM((max(segments), plan.cut, width), BF16),
            pltpu.VMEM((max(segments), plan.narrow_rows - plan.cut, width), F32),
            pltpu.VMEM((len(plan.narrow), kinds * width, kinds * width), BF16),
            pltpu.VMEM((crossing - 1, width, kinds * width), BF16),
            pltpu.VMEM((2 * width, 4 * width), BF16),
            pltpu.VMEM((4, blocks, width), F32),
            pltpu.VMEM((plan.wide_end, vectors, width), BF16),
            pltpu.VMEM((crossing, vectors, width), BF16),
            pltpu.VMEM((crossing, part, width), F32),
            pltpu.VMEM((crossing, vectors, width), BF16),
            pltpu.VMEM((2, vectors, width), BF16),
            pltpu.VMEM((2, vectors, width), BF16),
            pltpu.VMEM((near, crossing, part, width), BF16),
            pltpu.VMEM((crossing, part, width), BF16),
            pltpu.VMEM((near, part, width), BF16),
            pltpu.VMEM((far, crossing - 1, part, width), BF16),
            pltpu.VMEM((crossing - 1, part, width), BF16),
            pltpu.VMEM((near, crossing - 1, part, width), BF16),
            dma((near,)), dma((5,)),
            dma((near,)), dma((near,)), dma((near,)), dma((near,)), dma((far,)), dma((far,)), dma((near,)), dma((near,)), dma((2,)), dma((2,)),
        ],
        compiler_params=pltpu.CompilerParams(
            collective_id=0, has_side_effects=True, vmem_limit_bytes=VMEM_LIMIT),
        name="exchange",
    )(*pinned)

    pieces = [4] * (vectors // 4)
    return pl.pallas_call(
        functools.partial(final_kernel, plan, pieces),
        out_shape=jax.ShapeDtypeStruct(fine.shape, F32),
        in_specs=[vmem, vmem, vmem],
        out_specs=pl.BlockSpec(memory_space=pl.ANY),
        scratch_shapes=[pltpu.VMEM(fine.shape, F32), dma((len(pieces),))],
        compiler_params=pltpu.CompilerParams(vmem_limit_bytes=VMEM_LIMIT),
        name="final",
    )(spread, table, level0)


def solution(mesh):
    in_specs = (P(None, "gx", None), P(None, "gx"), P(), P(), P())
    out_specs = P(None, "gx", None)
    return jax.shard_map(shards, mesh=mesh, in_specs=in_specs, out_specs=out_specs, check_vma=False)
```
